128 devices in a mesh: seq: 16 (over y, z_lo, core), tensor: 8 (over z_hi, x).
Axes of the slice: x: 4, y: 4, z: 4 (z_hi: 2, z_lo: 2; z = z_hi * 2 + z_lo), core: 2. Of those that a mesh axis runs over, the one named last changes fastest.
Arguments:
- tokens: bfloat16 [8192, 8192], P('seq', 'tensor'), may hold values from -6 to 6
- positions: int32 [8192], P('seq'), may hold values from 0 to 8191, each once
- norm_gain: float32 [8192], replicated, may hold values from 0.1 to 1.9
- w_query: bfloat16 [8192, 4096], P('seq', 'tensor'), may hold values from -0.0625 to 0.0625
- w_key: bfloat16 [8192, 1024], P('seq', 'tensor'), may hold values from -0.0625 to 0.0625
- w_value: bfloat16 [8192, 1024], P('seq', 'tensor'), may hold values from -0.0625 to 0.0625
- b_query: float32 [4096], P('tensor'), may hold values from -40 to 40
- b_key: float32 [1024], P('tensor'), may hold values from -40 to 40
- b_value: float32 [1024], P('tensor'), may hold values from -6 to 6
- w_out: bfloat16 [4096, 8192], P('tensor', 'seq'), may hold values from -0.09375 to 0.09375
Outputs:
- mixed: bfloat16 [8192, 8192], P('seq', 'tensor')
- context: bfloat16 [8192, 4096], P('seq', 'tensor')
The draws below stay inside these ranges and needn't reach their ends.
Inputs may be any that keep to these rules, and one draw needn't show every extreme that they name: positions holds every position 0 to 8191 once.
All inputs are finite; a program needn't handle non-finite values.
Results may differ from the reference program's by a relative error of at most 0.025.
Values may be sent and summed in bfloat16 or wider, within the bound.
No kernel may reach another device: no remote copies, remote signals or barrier semaphores. Data moves between devices by JAX's collectives and lax.ppermute only.
A program may use at most 128 MiB of HBM per device.

```python
import jax
import jax.numpy as jnp
from jax import lax

D = 8192
HEADS = 32
KV_HEADS = 8
HD = 128
TOKENS = 8192


def draw_b_query(key, part):
    return jax.random.normal(jax.random.fold_in(key, 14), (HEADS * HD,), jnp.float32)


def draw_b_key(key, part):
    return jax.random.normal(jax.random.fold_in(key, 15), (KV_HEADS * HD,), jnp.float32)


def steps_of(rng, dims, cuts, low, high):
    factor_of, own = 1.0, jax.random.fold_in(rng, 6)
    for position, parts in cuts:
        steps = jnp.exp(jax.random.uniform(jax.random.fold_in(own, position), (parts,), jnp.float32, low / len(cuts), high / len(cuts)))
        factor_of = factor_of * jnp.repeat(steps, dims[position] // parts).reshape([-1 if axis == position else 1 for axis in range(len(dims))])
    return factor_of


def centred(own_key, dims, deviation, bound, split=(), held_as=jnp.bfloat16):
    loudness = steps_of(own_key, dims, split, -0.22, 0.18) if split else 1.0
    array = jax.random.normal(own_key, dims, jnp.float32) * deviation * loudness
    return jnp.minimum(jnp.maximum(array, -bound), bound).astype(held_as)


def setup_inputs(seed: int = 0) -> dict:
    splits = jax.random.split(jax.random.key(seed), 11)
    tokens = centred(splits[0], (TOKENS, D), 1.0, 6.0, ((0, 16), (1, 8)))
    positions = jax.random.permutation(splits[1], TOKENS).astype(jnp.int32)
    norm_gain = jnp.clip(1.0 + 0.18 * jax.random.normal(splits[2], (D,), jnp.float32), 0.1, 1.9)
    w_query = centred(splits[3], (D, HEADS * HD), D ** -0.5, 0.0625, ((0, 16), (1, 8)))
    w_key = centred(splits[4], (D, KV_HEADS * HD), D ** -0.5, 0.0625, ((0, 16), (1, 8)))
    w_value = centred(splits[5], (D, KV_HEADS * HD), D ** -0.5, 0.0625, ((0, 16), (1, 8)))
    b_query = draw_b_query(jax.random.fold_in(splits[10], 71), 0)
    b_key = draw_b_key(jax.random.fold_in(splits[10], 71), 0)
    b_value = centred(splits[8], (KV_HEADS * HD,), 1.0, 6.0, ((0, 8),), jnp.float32)
    w_out = centred(splits[9], (HEADS * HD, D), (HEADS * HD) ** -0.5, 0.09375, ((0, 8), (1, 16)))
    return dict(tokens=tokens, positions=positions, norm_gain=norm_gain, w_query=w_query, w_key=w_key, w_value=w_value, b_query=b_query, b_key=b_key, b_value=b_value, w_out=w_out)


NORM_EPS = 1e-06
ROPE_BASE = 1000000.0
NEG_FILL = -1e+30

def rotate(values_in, positions):
    half_dim = HD // 2
    inv_freq = ROPE_BASE ** (-jnp.arange(half_dim, dtype=jnp.float32) * 2.0 / HD)
    angles = positions.astype(jnp.float32)[:, None] * inv_freq[None, :]
    cosine = jnp.cos(angles)[:, None, :]
    sines = jnp.sin(angles)[:, None, :]
    lower_half = values_in[..., :half_dim]
    upper_half = values_in[..., half_dim:]
    return jnp.concatenate([lower_half * cosine - upper_half * sines, upper_half * cosine + lower_half * sines], -1)

def reference(tokens, positions, norm_gain, w_query, w_key, w_value, b_query, b_key, b_value, w_out):
    group = HEADS // KV_HEADS
    inputs = tokens.astype(jnp.float32)
    inverse_rms = lax.rsqrt(lax.optimization_barrier(jnp.mean(inputs * inputs, -1, keepdims=True)) + NORM_EPS)
    normed = (inputs * inverse_rms * norm_gain.astype(jnp.float32)[None, :]).astype(jnp.bfloat16)
    q_proj = jnp.dot(normed, w_query, preferred_element_type=jnp.float32) + b_query.astype(jnp.float32)[None, :]
    k_proj = jnp.dot(normed, w_key, preferred_element_type=jnp.float32) + b_key.astype(jnp.float32)[None, :]
    v_proj = jnp.dot(normed, w_value, preferred_element_type=jnp.float32) + b_value.astype(jnp.float32)[None, :]
    queries = rotate(q_proj.reshape(TOKENS, HEADS, HD), positions).astype(jnp.bfloat16)
    keys_rot = rotate(k_proj.reshape(TOKENS, KV_HEADS, HD), positions).astype(jnp.bfloat16)
    values = v_proj.astype(jnp.bfloat16).reshape(TOKENS, KV_HEADS, HD)
    queries = jnp.moveaxis(queries, 1, 0)
    keys_rot = jnp.moveaxis(keys_rot, 1, 0)
    values = jnp.moveaxis(values, 1, 0)
    allowed = positions[None, :] <= positions[:, None]
    scale = HD ** (-0.5)

    def one_head(head_index):
        q_head = lax.dynamic_index_in_dim(queries, head_index, 0, keepdims=False).astype(jnp.float32)
        kv_index = head_index // group
        k_head = lax.dynamic_index_in_dim(keys_rot, kv_index, 0, keepdims=False).astype(jnp.float32)
        v_head = lax.dynamic_index_in_dim(values, kv_index, 0, keepdims=False)
        scores = jnp.dot(q_head, k_head.T) * scale
        scores = jnp.where(allowed, scores, NEG_FILL)
        row_max = lax.optimization_barrier(jnp.max(scores, -1, keepdims=True))
        weights = jnp.where(allowed, jnp.exp(scores - row_max), 0.0)
        denominator = lax.optimization_barrier(jnp.sum(weights, -1, keepdims=True))
        numerator = jnp.dot(weights.astype(jnp.bfloat16), v_head, preferred_element_type=jnp.float32)
        return (numerator / denominator).astype(jnp.bfloat16)
    per_head = lax.map(one_head, jnp.arange(HEADS, dtype=jnp.int32))
    context = jnp.moveaxis(per_head, 0, 1).reshape(TOKENS, HEADS * HD)
    mixed = (inputs + jnp.dot(context, w_out, preferred_element_type=jnp.float32)).astype(jnp.bfloat16)
    return (mixed, context)
```

```python
import math

import jax
import jax.numpy as jnp
from jax import lax
from jax.experimental import pallas as pl
from jax.experimental.pallas import tpu as pltpu
from jax.sharding import Mesh, PartitionSpec as P

HD = 128
NORM_EPS = 1e-06
ROPE_BASE = 1000000.0
NEG_FILL = -1e30
SEQ = ("y", "zl", "core")
TENSOR = ("zh", "x")
ROWS = 512
FEAT = 1024
MODEL = 8192
SOURCES = 16
GROUPS = 8
HEADS = 4
POS_ROWS = 16
KSTEP = 32
NSTEPS = ROWS // KSTEP
CHUNKS = 2
CROWS = ROWS // CHUNKS
QSCALE = HD**-0.5 * math.log2(math.e)


NEXT = [(i, (i + 1) % 4) for i in range(4)]
PREV = [(i, (i - 1) % 4) for i in range(4)]
ACROSS = [(i, (i + 2) % 4) for i in range(4)]
SWAP = [(0, 1), (1, 0)]


def project_body(n_pieces, queries, ids, *refs):
    pieces = refs[: len(n_pieces)]
    w_ref, bias_ref, cos_ref, sin_ref, out_ref, tbuf, acc, square, sems = refs[len(n_pieces) :]
    step = pl.program_id(0)

    def fetch(i):
        slot, start, size = n_pieces[i]
        return pltpu.make_async_copy(pieces[i], tbuf.at[slot, pl.ds(start, size)], sems.at[i])

    @pl.when(step == 0)
    def _():
        for i in range(len(n_pieces)):
            fetch(i).start()
        acc[...] = jnp.zeros_like(acc)
        square[...] = jnp.zeros_like(square)

    for k in range(GROUPS):

        @pl.when(step == k)
        def _(k=k):
            for i, (slot, _, _) in enumerate(n_pieces):
                if slot == k:
                    fetch(i).wait()

    rows = tbuf[step]
    half = FEAT // 2
    acc[...] += jnp.dot(rows[:, :half], w_ref[0], preferred_element_type=jnp.float32) + jnp.dot(
        rows[:, half:], w_ref[1], preferred_element_type=jnp.float32
    )
    wide = rows.astype(jnp.float32)
    wide = wide * wide
    total = wide[:, :HD]
    for i in range(1, FEAT // HD):
        total = total + wide[:, i * HD : (i + 1) * HD]
    square[...] += total

    @pl.when(step == GROUPS - 1)
    def _():
        mean = jnp.sum(square[...], axis=1, keepdims=True) * (1.0 / MODEL)
        inverse = lax.rsqrt(mean + NORM_EPS)
        cosine = cos_ref[...]
        sines = sin_ref[...]

        def head(i):
            return acc[:, i * HD : (i + 1) * HD] * inverse + bias_ref[:, i * HD : (i + 1) * HD]

        def turned(u):
            return u * cosine + pltpu.roll(u, HD // 2, 1) * sines

        if queries:
            for i in range(HEADS):
                out_ref[i] = (turned(head(i)) * QSCALE).astype(jnp.bfloat16)
        else:
            out_ref[:, :HD] = turned(head(0)).astype(jnp.bfloat16)
            out_ref[:, HD:] = head(1).astype(jnp.bfloat16)


def project(pieces, slots, ids, weights, bias, cosine, sines, queries):
    width = HEADS * HD if queries else 2 * HD
    column = 0 if queries else HEADS // 2
    out_shape = (HEADS, ROWS, HD) if queries else (ROWS, 2 * HD)

    def body(*refs):
        project_body(slots, queries, *refs)

    def whole(*shape):
        return pl.BlockSpec(shape, lambda k, ids: (0,) * len(shape))

    return pl.pallas_call(
        body,
        grid_spec=pltpu.PrefetchScalarGridSpec(
            num_scalar_prefetch=1,
            grid=(GROUPS,),
            in_specs=[pl.BlockSpec(memory_space=pl.ANY)] * len(pieces)
            + [
                pl.BlockSpec((2, ROWS, width), lambda k, ids: (ids[k], 0, column)),
                whole(1, width),
                whole(ROWS, HD),
                whole(ROWS, HD),
            ],
            out_specs=whole(*out_shape),
            scratch_shapes=[
                pltpu.VMEM((GROUPS, ROWS, FEAT), jnp.bfloat16),
                pltpu.VMEM((ROWS, width), jnp.float32),
                pltpu.VMEM((ROWS, HD), jnp.float32),
                pltpu.SemaphoreType.DMA((len(pieces),)),
            ],
        ),
        out_shape=jax.ShapeDtypeStruct(out_shape, jnp.bfloat16),
        compiler_params=pltpu.CompilerParams(dimension_semantics=("arbitrary",)),
        name="project_queries" if queries else "project_keys",
    )(ids, *pieces, weights, bias, cosine, sines)


def attend_body(bounds, q_ref, qpos_ref, kv_ref, kpos_ref, out_ref, top, acc):
    chunk = pl.program_id(0)
    full = bounds[0, chunk]
    need = bounds[1, chunk]
    top[...] = jnp.full_like(top, NEG_FILL)
    acc[...] = jnp.zeros_like(acc)
    ones = jnp.ones((SOURCES * KSTEP, HD), jnp.bfloat16)
    rows = q_ref.shape[1]

    def one_step(j, masked):
        at = pl.multiple_of(j * KSTEP, KSTEP)
        block = kv_ref[:, pl.ds(at, KSTEP), :].reshape(SOURCES * KSTEP, 2 * HD)
        keys = block[:, :HD]
        values = jnp.concatenate([block[:, HD:], ones], axis=1)
        for h in range(HEADS):
            scores = lax.dot_general(
                q_ref[h], keys, (((1,), (1,)), ((), ())), preferred_element_type=jnp.float32
            )
            if masked:
                allowed = kpos_ref[j] <= qpos_ref[...]
                scores = jnp.where(allowed, scores, NEG_FILL)
            old = top[h]
            new = jnp.maximum(old, jnp.max(scores, axis=1, keepdims=True))
            weights = jnp.exp2(scores - new[:, :1]).astype(jnp.bfloat16)
            rescale = jnp.exp2(old - new)
            top[h] = new
            acc[h] = acc[h] * jnp.concatenate([rescale, rescale], axis=1) + jnp.dot(
                weights, values, preferred_element_type=jnp.float32
            )

    def unmasked(j, carry):
        one_step(j, False)
        return carry

    def masked(j, carry):
        one_step(j, True)
        return carry

    lax.fori_loop(0, full, unmasked, 0)
    lax.fori_loop(full, need, masked, 0)
    for h in range(HEADS):
        out_ref[:, h * HD : (h + 1) * HD] = (acc[h, :, :HD] / acc[h, :, HD:]).astype(jnp.bfloat16)


def attend(bounds, queries, qpos, kv, kpos, first, count, rows):
    def whole(*shape):
        return pl.BlockSpec(shape, lambda c, b: (0,) * len(shape))

    return pl.pallas_call(
        attend_body,
        grid_spec=pltpu.PrefetchScalarGridSpec(
            num_scalar_prefetch=1,
            grid=(count,),
            in_specs=[
                pl.BlockSpec((HEADS, rows, HD), lambda c, b: (0, c + first, 0)),
                pl.BlockSpec((rows, 1), lambda c, b: (c + first, 0)),
                whole(SOURCES, ROWS, 2 * HD),
                whole(NSTEPS, 1, SOURCES * KSTEP),
            ],
            out_specs=pl.BlockSpec((rows, HEADS * HD), lambda c, b: (c, 0)),
            scratch_shapes=[
                pltpu.VMEM((HEADS, rows, HD), jnp.float32),
                pltpu.VMEM((HEADS, rows, 2 * HD), jnp.float32),
            ],
        ),
        out_shape=jax.ShapeDtypeStruct((rows * count, HEADS * HD), jnp.bfloat16),
        compiler_params=pltpu.CompilerParams(dimension_semantics=("arbitrary",)),
        name=f"attend_{first}",
    )(bounds, queries, qpos, kv, kpos)


def mix_body(slots, ids, *refs):
    pieces = refs[: len(slots)]
    w_ref, back_ref, tokens_ref, out_ref, cbuf, acc, sems = refs[len(slots) :]
    step = pl.program_id(0)

    def fetch(i):
        slot, start, size = slots[i]
        return pltpu.make_async_copy(pieces[i], cbuf.at[slot, pl.ds(start, size)], sems.at[i])

    @pl.when(step == 0)
    def _():
        for i in range(len(slots)):
            fetch(i).start()
        acc[...] = jnp.zeros_like(acc)

    for k in range(GROUPS):

        @pl.when(step == k)
        def _(k=k):
            for i, (slot, _, _) in enumerate(slots):
                if slot == k:
                    fetch(i).wait()

    rows = cbuf[step]
    for half in range(2):
        cols = slice(half * 512, (half + 1) * 512)
        acc[:, cols] += jnp.dot(rows, w_ref[half], preferred_element_type=jnp.float32)

    @pl.when(step == GROUPS - 1)
    def _():
        back = back_ref[...]
        high = acc[...].astype(jnp.bfloat16)
        low = (acc[...] - high.astype(jnp.float32)).astype(jnp.bfloat16)
        mixed = jnp.dot(back, high, preferred_element_type=jnp.float32) + jnp.dot(
            back, low, preferred_element_type=jnp.float32
        )
        out_ref[...] = (tokens_ref[...].astype(jnp.float32) + mixed).astype(jnp.bfloat16)


def mix(pieces, slots, ids, w_out, back, tokens):
    def body(*refs):
        mix_body(slots, *refs)

    def whole(*shape):
        return pl.BlockSpec(shape, lambda k, ids: (0,) * len(shape))

    return pl.pallas_call(
        body,
        grid_spec=pltpu.PrefetchScalarGridSpec(
            num_scalar_prefetch=1,
            grid=(GROUPS,),
            in_specs=[pl.BlockSpec(memory_space=pl.ANY)] * len(pieces)
            + [
                pl.BlockSpec((2, ROWS, 512), lambda k, ids: (ids[k], 0, 0)),
                whole(ROWS, ROWS),
                whole(ROWS, FEAT),
            ],
            out_specs=whole(ROWS, FEAT),
            scratch_shapes=[
                pltpu.VMEM((GROUPS, ROWS, HEADS * HD), jnp.bfloat16),
                pltpu.VMEM((ROWS, FEAT), jnp.float32),
                pltpu.SemaphoreType.DMA((len(pieces),)),
            ],
        ),
        out_shape=jax.ShapeDtypeStruct((ROWS, FEAT), jnp.bfloat16),
        compiler_params=pltpu.CompilerParams(dimension_semantics=("arbitrary",)),
        name="mix",
    )(ids, *pieces, w_out, back, tokens)


def shards(tokens, positions, norm_gain, w_query, w_key, w_value, b_query, b_key, b_value, w_out):
    bf16, f32 = (jnp.bfloat16, jnp.float32)
    seq_at = lax.axis_index(SEQ)
    zh, x = (lax.axis_index("zh"), lax.axis_index("x"))

    rank = jnp.sum((positions[None, :] < positions[:, None]).astype(jnp.int32), 1)
    chosen = rank[None, :] == jnp.arange(ROWS, dtype=jnp.int32)[:, None]
    order = chosen.astype(bf16)
    back = (rank[:, None] == jnp.arange(ROWS, dtype=jnp.int32)[None, :]).astype(bf16)
    sorted_pos = jnp.sum(jnp.where(chosen, positions[None, :], 0), 1)
    sorted_tokens = jnp.dot(order, tokens, preferred_element_type=f32).astype(bf16)

    w_cat = jnp.concatenate((w_query, w_key, w_value), 1)
    gain = lax.dynamic_slice(norm_gain, (seq_at * ROWS,), (ROWS,))
    w_cat = (w_cat.astype(f32) * gain[:, None]).astype(bf16)
    width = w_cat.shape[1]
    pos_rows = jnp.stack([sorted_pos >> 7, sorted_pos & 127]).astype(bf16)
    pos_rows = jnp.pad(pos_rows, ((0, POS_ROWS - 2), (0, width - ROWS)))
    weights = lax.all_gather(jnp.concatenate([w_cat, pos_rows], 0), SEQ, axis=0, tiled=True)
    weights = weights.reshape(SOURCES, ROWS + POS_ROWS, width)

    def ring(own):
        half = own.shape[0] // 2
        left = lax.ppermute(own, "x", NEXT)
        right = lax.ppermute(own, "x", PREV)
        low = lax.ppermute(left[:half], "x", NEXT)
        high = lax.ppermute(right[half:], "x", PREV)
        return left, right, low, high

    left, right, low, high = ring(sorted_tokens)
    other = lax.ppermute(sorted_tokens, "zh", SWAP)
    oleft = lax.ppermute(other, "x", NEXT)
    oright = lax.ppermute(other, "x", PREV)
    olow = lax.ppermute(low, "zh", SWAP)
    ohigh = lax.ppermute(high, "zh", SWAP)
    ids = jnp.stack(
        [z * 4 + (x + d) % 4 for z in (zh, 1 - zh) for d in (0, 3, 1, 2)]
    ).astype(jnp.int32)
    ids = ids[jnp.array([0, 1, 2, 4, 3, 5, 6, 7])]
    half = ROWS // 2
    pieces = [sorted_tokens, left, right, other, low, high, oleft, oright, olow, ohigh]
    slots = [
        (0, 0, ROWS),
        (1, 0, ROWS),
        (2, 0, ROWS),
        (3, 0, ROWS),
        (4, 0, half),
        (4, half, half),
        (5, 0, ROWS),
        (6, 0, ROWS),
        (7, 0, half),
        (7, half, half),
    ]

    half_dim = HD // 2
    inv_freq = ROPE_BASE ** (-jnp.arange(half_dim, dtype=f32) * 2.0 / HD)
    angles = sorted_pos.astype(f32)[:, None] * inv_freq[None, :]
    cosine = jnp.cos(angles)
    sines = jnp.sin(angles)
    cosine = jnp.concatenate([cosine, cosine], 1)
    sines = jnp.concatenate([-sines, sines], 1)

    kv_bias = jnp.concatenate((b_key, b_value))[None, :]
    kv = project(pieces, slots, ids, weights, kv_bias, cosine, sines, False)
    kv_all = lax.all_gather(kv, SEQ, axis=0, tiled=True).reshape(SOURCES, ROWS, 2 * HD)
    queries = project(pieces, slots, ids, weights, b_query[None, :], cosine, sines, True)

    swap = [
        ((a * 2 + core) * 8 + b, (b * 2 + core) * 8 + a)
        for a in range(8)
        for core in range(2)
        for b in range(8)
    ]
    moved = lax.ppermute(w_out, SEQ + TENSOR, swap)
    w_out_all = lax.all_gather(moved, SEQ, axis=0, tiled=True).reshape(SOURCES, 512, 512)

    pos_all = weights[:, ROWS : ROWS + 2, :ROWS].astype(jnp.int32)
    pos_all = pos_all[:, 0] * 128 + pos_all[:, 1]
    kpos = pos_all.reshape(SOURCES, NSTEPS, KSTEP).transpose(1, 0, 2)
    first_pos = jnp.min(kpos, (1, 2))
    last_pos = jnp.max(kpos, (1, 2))
    kpos = kpos.reshape(NSTEPS, 1, SOURCES * KSTEP)
    by_chunk = sorted_pos.reshape(CHUNKS, CROWS)
    full = jnp.sum((last_pos[None, :] <= by_chunk[:, :1]).astype(jnp.int32), 1)
    need = jnp.sum((first_pos[None, :] <= by_chunk[:, -1:]).astype(jnp.int32), 1)
    bounds = jnp.stack([full, need])

    mix_pieces, mix_slots, contexts = ([], [], [])
    for c in range(CHUNKS):
        context = attend(bounds[:, c : c + 1], queries, sorted_pos[:, None], kv_all, kpos, c, 1, CROWS)
        contexts.append(context)
        across = lax.ppermute(context, "zh", SWAP)
        for z, own in enumerate((context, across)):
            found = [
                own,
                lax.ppermute(own, "x", NEXT),
                lax.ppermute(own, "x", PREV),
                lax.ppermute(own, "x", ACROSS),
            ]
            mix_pieces += found
            mix_slots += [(z * 4 + i, c * CROWS, CROWS) for i in range(4)]
    mix_ids = jnp.stack(
        [z * 4 + (x + d) % 4 for z in (zh, 1 - zh) for d in (0, 3, 1, 2)]
    ).astype(jnp.int32)
    mixed = mix(mix_pieces, mix_slots, mix_ids, w_out_all, back, tokens)
    context = jnp.dot(back, jnp.concatenate(contexts, 0), preferred_element_type=f32).astype(bf16)
    return (mixed, context)


def solution(mesh):
    fine = Mesh(mesh.devices.reshape(4, 2, 2, 2, 4), SEQ + TENSOR)
    in_specs = (
        P(SEQ, TENSOR),
        P(SEQ),
        P(),
        P(SEQ, TENSOR),
        P(SEQ, TENSOR),
        P(SEQ, TENSOR),
        P(TENSOR),
        P(TENSOR),
        P(TENSOR),
        P(TENSOR, SEQ),
    )
    out_specs = (P(SEQ, TENSOR), P(SEQ, TENSOR))
    return jax.shard_map(shards, mesh=fine, in_specs=in_specs, out_specs=out_specs, check_vma=False)
```

```python
import math

import jax
import jax.numpy as jnp
from jax import lax
from jax.experimental import pallas as pl
from jax.experimental.pallas import tpu as pltpu
from jax.sharding import Mesh, PartitionSpec as P


HD = 128
NORM_EPS = 1e-06
ROPE_BASE = 1000000.0
NEG_FILL = -1e30
SEQ = ("y", "zl", "core")
TENSOR = ("zh", "x")
ROWS = 512
FEAT = 1024
MODEL = 8192
SOURCES = 16
GROUPS = 8
HEADS = 4
POS_ROWS = 16
KSTEP = 64
NSTEPS = ROWS // KSTEP
KEYS = SOURCES * KSTEP
BLOCK = 128
BLOCKS = ROWS // BLOCK
CALLS = ((0, 2), (2, 2))
PER_STEP = 2
QSCALE = HD**-0.5 * math.log2(math.e)


NEXT = [(i, (i + 1) % 4) for i in range(4)]
PREV = [(i, (i - 1) % 4) for i in range(4)]
ACROSS = [(i, (i + 2) % 4) for i in range(4)]
SWAP = [(0, 1), (1, 0)]


def fetch_all(pieces, slots, buffer, sems, step):
    def fetch(i):
        slot, start, size = slots[i]
        return pltpu.make_async_copy(pieces[i], buffer.at[slot, pl.ds(start, size)], sems.at[i])

    @pl.when(step == 0)
    def _():
        for i in range(len(slots)):
            fetch(i).start()

    for k in range(GROUPS // PER_STEP):

        @pl.when(step == k)
        def _(k=k):
            for i, (slot, _, _) in enumerate(slots):
                if slot // PER_STEP == k:
                    fetch(i).wait()


def whole(*shape):
    return pl.BlockSpec(shape, lambda k, ids: (0,) * len(shape))


def project_body(slots, queries, ids, *refs):
    pieces = refs[: len(slots)]
    refs = refs[len(slots) :]
    w_refs = refs[:PER_STEP]
    inverse_ref, bias_ref, cos_ref, sin_ref, out_ref, tbuf, acc, sems = refs[PER_STEP:]
    step = pl.program_id(0)
    fetch_all(pieces, slots, tbuf, sems, step)
    half = FEAT // 2
    total = None
    for i in range(PER_STEP):
        rows = tbuf[step * PER_STEP + i]
        for j in range(2):
            part = jnp.dot(
                rows[:, j * half : (j + 1) * half], w_refs[i][j], preferred_element_type=jnp.float32
            )
            total = part if total is None else total + part

    @pl.when(step == 0)
    def _():
        acc[...] = total

    @pl.when(step > 0)
    def _():
        acc[...] += total

    @pl.when(step == GROUPS // PER_STEP - 1)
    def _():
        inverse = inverse_ref[...]
        cosine = cos_ref[...]
        sines = sin_ref[...]

        def head(i):
            return acc[:, i * HD : (i + 1) * HD] * inverse + bias_ref[:, i * HD : (i + 1) * HD]

        def turned(u):
            return u * cosine + pltpu.roll(u, HD // 2, 1) * sines

        if queries:
            for i in range(HEADS):
                q = (turned(head(i)) * QSCALE).astype(jnp.bfloat16)
                for b in range(BLOCKS):
                    out_ref[b, i * BLOCK : (i + 1) * BLOCK] = q[b * BLOCK : (b + 1) * BLOCK]
        else:
            out_ref[:, :HD] = turned(head(0)).astype(jnp.bfloat16)
            out_ref[:, HD:] = head(1).astype(jnp.bfloat16)


def w_spec(i, width, column):
    return pl.BlockSpec((2, ROWS, width), lambda k, ids: (ids[k * PER_STEP + i], 0, column))


def project(pieces, slots, ids, weights, inverse, bias, cosine, sines, queries):
    width = HEADS * HD if queries else 2 * HD
    column = 0 if queries else HEADS // 2
    out_shape = (BLOCKS, HEADS * BLOCK, HD) if queries else (ROWS, 2 * HD)

    def body(*refs):
        project_body(slots, queries, *refs)

    return pl.pallas_call(
        body,
        grid_spec=pltpu.PrefetchScalarGridSpec(
            num_scalar_prefetch=1,
            grid=(GROUPS // PER_STEP,),
            in_specs=[pl.BlockSpec(memory_space=pl.ANY)] * len(pieces)
            + [w_spec(i, width, column) for i in range(PER_STEP)]
            + [whole(ROWS, 1), whole(1, width), whole(ROWS, HD), whole(ROWS, HD)],
            out_specs=whole(*out_shape),
            scratch_shapes=[
                pltpu.VMEM((GROUPS, ROWS, FEAT), jnp.bfloat16),
                pltpu.VMEM((ROWS, width), jnp.float32),
                pltpu.SemaphoreType.DMA((len(pieces),)),
            ],
        ),
        out_shape=jax.ShapeDtypeStruct(out_shape, jnp.bfloat16),
        compiler_params=pltpu.CompilerParams(dimension_semantics=("arbitrary",)),
        cost_estimate=pl.CostEstimate(
            flops=2 * ROWS * MODEL * width, transcendentals=0, bytes_accessed=16 << 20
        ),
        name="project_queries" if queries else "project_keys",
    )(ids, *pieces, *([weights] * PER_STEP), inverse, bias, cosine, sines)


def attend_body(bounds, q_ref, qpos_ref, own_ref, other_ref, kpos_ref, out_ref, kv_ref, top, acc, sems):
    block_at = pl.program_id(0)
    full = bounds[0, block_at]
    need = bounds[1, block_at]

    def fetch(i):
        source = (own_ref, other_ref)[i]
        half = SOURCES // 2
        return pltpu.make_async_copy(source, kv_ref.at[pl.ds(i * half, half)], sems.at[i])

    @pl.when(block_at == 0)
    def _():
        fetch(0).start()
        fetch(1).start()

    top[...] = jnp.full_like(top, NEG_FILL)
    acc[...] = jnp.zeros_like(acc)

    @pl.when(block_at == 0)
    def _():
        fetch(0).wait()
        fetch(1).wait()

    ones = jnp.ones((KEYS, HD), jnp.bfloat16)
    parts = top.shape[0]
    rows = top.shape[1]

    def one_step(j, masked):
        at = pl.multiple_of(j * KSTEP, KSTEP)
        block = kv_ref[:, pl.ds(at, KSTEP), :].reshape(KEYS, 2 * HD)
        keys = block[:, :HD]
        values = jnp.concatenate([block[:, HD:], ones], axis=1)

        def scores_of(h):
            return lax.dot_general(
                q_ref[0, h * rows : (h + 1) * rows],
                keys,
                (((1,), (1,)), ((), ())),
                preferred_element_type=jnp.float32,
            )

        following = scores_of(0)
        for h in range(parts):
            scores = following
            following = scores_of(h + 1) if h + 1 < parts else None
            if masked:
                allowed = kpos_ref[j] <= qpos_ref[0, h * rows : (h + 1) * rows]
                scores = jnp.where(allowed, scores, NEG_FILL)
            old = top[h]
            new = jnp.maximum(old, jnp.max(scores, axis=1, keepdims=True))
            weights = jnp.exp2(scores - jnp.concatenate([new] * (KEYS // HD), axis=1))
            rescale = jnp.exp2(old - new)
            top[h] = new
            acc[h] = acc[h] * jnp.concatenate([rescale, rescale], axis=1) + jnp.dot(
                weights.astype(jnp.bfloat16), values, preferred_element_type=jnp.float32
            )

    def unmasked(j, carry):
        one_step(j, False)
        return carry

    def masked(j, carry):
        one_step(j, True)
        return carry

    lax.fori_loop(0, full, unmasked, 0)
    lax.fori_loop(full, need, masked, 0)
    for h in range(HEADS):
        part, at = (h * BLOCK // rows, h * BLOCK % rows)
        done = acc[part, at : at + BLOCK, :HD] / acc[part, at : at + BLOCK, HD:]
        out_ref[:, h * HD : (h + 1) * HD] = done.astype(jnp.bfloat16)


def attend(bounds, queries, qpos, own, other, kpos, first, count):
    part = 2 * BLOCK
    return pl.pallas_call(
        attend_body,
        grid_spec=pltpu.PrefetchScalarGridSpec(
            num_scalar_prefetch=1,
            grid=(count,),
            in_specs=[
                pl.BlockSpec((1, HEADS * BLOCK, HD), lambda c, b: (c + first, 0, 0)),
                pl.BlockSpec((1, HEADS * BLOCK, 1), lambda c, b: (c + first, 0, 0)),
                pl.BlockSpec(memory_space=pl.ANY),
                pl.BlockSpec(memory_space=pl.ANY),
                whole(NSTEPS, 1, KEYS),
            ],
            out_specs=pl.BlockSpec((BLOCK, HEADS * HD), lambda c, b: (c, 0)),
            scratch_shapes=[
                pltpu.VMEM((SOURCES, ROWS, 2 * HD), jnp.bfloat16),
                pltpu.VMEM((HEADS * BLOCK // part, part, HD), jnp.float32),
                pltpu.VMEM((HEADS * BLOCK // part, part, 2 * HD), jnp.float32),
                pltpu.SemaphoreType.DMA((2,)),
            ],
        ),
        out_shape=jax.ShapeDtypeStruct((BLOCK * count, HEADS * HD), jnp.bfloat16),
        compiler_params=pltpu.CompilerParams(dimension_semantics=("arbitrary",)),
        cost_estimate=pl.CostEstimate(
            flops=4 * HEADS * BLOCK * count * SOURCES * ROWS * HD,
            transcendentals=HEADS * BLOCK * count * SOURCES * ROWS,
            bytes_accessed=6 << 20,
        ),
    )(bounds, queries, qpos, own, other, kpos)


def mix_body(slots, ids, *refs):
    pieces = refs[: len(slots)]
    refs = refs[len(slots) :]
    w_refs = refs[:PER_STEP]
    back_ref, base_ref, out_ref, cbuf, acc, sems = refs[PER_STEP:]
    step = pl.program_id(0)
    fetch_all(pieces, slots, cbuf, sems, step)
    parts = []
    for half in range(2):
        total = None
        for i in range(PER_STEP):
            part = jnp.dot(
                cbuf[step * PER_STEP + i], w_refs[i][half], preferred_element_type=jnp.float32
            )
            total = part if total is None else total + part
        parts.append(total)

    @pl.when(step == 0)
    def _():
        for half in range(2):
            acc[:, half * 512 : (half + 1) * 512] = parts[half]

    @pl.when(step > 0)
    def _():
        for half in range(2):
            acc[:, half * 512 : (half + 1) * 512] += parts[half]

    @pl.when(step == GROUPS // PER_STEP - 1)
    def _():
        back = back_ref[...]
        high = acc[...].astype(jnp.bfloat16)
        low = (acc[...] - high.astype(jnp.float32)).astype(jnp.bfloat16)
        mixed = jnp.dot(back, high, preferred_element_type=jnp.float32) + jnp.dot(
            back, low, preferred_element_type=jnp.float32
        )
        out_ref[...] = (base_ref[...].astype(jnp.float32) + mixed).astype(out_ref.dtype)


def mix(pieces, ids, w_out, back, base, last):
    rows = pieces[0].shape[0]
    slots = [(i, 0, rows) for i in range(GROUPS)]

    def body(*refs):
        mix_body(slots, *refs)

    return pl.pallas_call(
        body,
        grid_spec=pltpu.PrefetchScalarGridSpec(
            num_scalar_prefetch=1,
            grid=(GROUPS // PER_STEP,),
            in_specs=[pl.BlockSpec(memory_space=pl.ANY)] * len(pieces)
            + [w_spec(i, 512, 0) for i in range(PER_STEP)]
            + [whole(ROWS, rows), whole(ROWS, FEAT)],
            out_specs=whole(ROWS, FEAT),
            scratch_shapes=[
                pltpu.VMEM((GROUPS, rows, HEADS * HD), jnp.bfloat16),
                pltpu.VMEM((rows, FEAT), jnp.float32),
                pltpu.SemaphoreType.DMA((len(pieces),)),
            ],
        ),
        out_shape=jax.ShapeDtypeStruct((ROWS, FEAT), jnp.bfloat16 if last else jnp.float32),
        compiler_params=pltpu.CompilerParams(dimension_semantics=("arbitrary",)),
        cost_estimate=pl.CostEstimate(
            flops=2 * rows * HEADS * HD * GROUPS * FEAT, transcendentals=0, bytes_accessed=12 << 20
        ),
        name="mix_last" if last else "mix_first",
    )(ids, *pieces, *([w_out] * PER_STEP), back, base)


def block(tokens, positions, norm_gain, w_query, w_key, w_value, b_query, b_key, b_value, w_out):
    bf16, f32 = (jnp.bfloat16, jnp.float32)
    seq_at = lax.axis_index(SEQ)
    zh, x = (lax.axis_index("zh"), lax.axis_index("x"))

    rank = jnp.sum((positions[None, :] < positions[:, None]).astype(jnp.int32), 1)
    chosen = rank[None, :] == jnp.arange(ROWS, dtype=jnp.int32)[:, None]
    order = chosen.astype(bf16)
    back = (rank[:, None] == jnp.arange(ROWS, dtype=jnp.int32)[None, :]).astype(bf16)
    sorted_pos = jnp.sum(jnp.where(chosen, positions[None, :], 0), 1)
    sorted_tokens = jnp.dot(order, tokens, preferred_element_type=f32).astype(bf16)

    w_cat = jnp.concatenate((w_query, w_key, w_value), 1)
    gain = lax.dynamic_slice(norm_gain, (seq_at * ROWS,), (ROWS,))
    w_cat = (w_cat.astype(f32) * gain[:, None]).astype(bf16)
    width = w_cat.shape[1]
    pos_rows = jnp.stack([sorted_pos >> 7, sorted_pos & 127]).astype(bf16)
    pos_rows = jnp.pad(pos_rows, ((0, POS_ROWS - 2), (0, width - ROWS)))
    weights = lax.all_gather(jnp.concatenate([w_cat, pos_rows], 0), SEQ, axis=0, tiled=True)
    weights = weights.reshape(SOURCES, ROWS + POS_ROWS, width)

    def ring(own):
        half = own.shape[0] // 2
        left = lax.ppermute(own, "x", NEXT)
        right = lax.ppermute(own, "x", PREV)
        low, high = (left[:half], right[half:])
        low = lax.ppermute(low, "x", NEXT)
        high = lax.ppermute(high, "x", PREV)
        return left, right, low, high

    other = lax.ppermute(sorted_tokens, "zh", SWAP)
    left, right, low, high = ring(sorted_tokens)
    oleft, oright, olow, ohigh = ring(other)

    def square(piece):
        wide = piece.astype(f32)
        return jnp.sum(wide * wide, 1, keepdims=True)

    total = sum(square(p) for p in (sorted_tokens, left, right, other, oleft, oright))
    total += jnp.concatenate([square(low), square(high)], 0)
    total += jnp.concatenate([square(olow), square(ohigh)], 0)
    inverse = lax.rsqrt(total * (1.0 / MODEL) + NORM_EPS)
    ids = jnp.stack(
        [z * 4 + (x + d) % 4 for z in (zh, 1 - zh) for d in (0, 3, 1, 2)]
    ).astype(jnp.int32)
    ids = ids[jnp.array([0, 1, 2, 4, 3, 5, 6, 7])]
    half = ROWS // 2
    pieces = [sorted_tokens, left, right, other, low, high, oleft, oright, olow, ohigh]
    slots = [
        (0, 0, ROWS),
        (1, 0, ROWS),
        (2, 0, ROWS),
        (3, 0, ROWS),
        (4, 0, half),
        (4, half, half),
        (5, 0, ROWS),
        (6, 0, ROWS),
        (7, 0, half),
        (7, half, half),
    ]

    half_dim = HD // 2
    inv_freq = ROPE_BASE ** (-jnp.arange(half_dim, dtype=f32) * 2.0 / HD)
    angles = sorted_pos.astype(f32)[:, None] * inv_freq[None, :]
    cosine = jnp.cos(angles)
    sines = jnp.sin(angles)
    cosine = jnp.concatenate([cosine, cosine], 1)
    sines = jnp.concatenate([-sines, sines], 1)

    kv_bias = jnp.concatenate((b_key, b_value))[None, :]
    kv = project(pieces, slots, ids, weights, inverse, kv_bias, cosine, sines, False)

    def flipped(steps):
        turn = dict(steps)
        return [(a * 2 + b, turn[a] * 2 + 1 - b) for a in range(4) for b in range(2)]

    found = [kv, lax.ppermute(kv, "zl", SWAP)]
    found += [lax.ppermute(kv, "y", steps) for steps in (NEXT, PREV, ACROSS)]
    found += [lax.ppermute(kv, ("y", "zl"), flipped(steps)) for steps in (NEXT, PREV, ACROSS)]
    own_kv = jnp.stack(found)
    other_kv = lax.ppermute(own_kv, "core", SWAP)
    y, zl, core = (lax.axis_index("y"), lax.axis_index("zl"), lax.axis_index("core"))
    chips = [y * 2 + zl, y * 2 + 1 - zl]
    chips += [(y + d) % 4 * 2 + z for z in (zl, 1 - zl) for d in (3, 1, 2)]
    sources = jnp.stack([chip * 2 + c for c in (core, 1 - core) for chip in chips])

    queries = project(
        pieces, slots, ids, weights, inverse, b_query[None, :], cosine, sines, True
    )

    pos_all = weights[:, ROWS : ROWS + 2, :ROWS].astype(jnp.int32)
    pos_all = pos_all[:, 0] * 128 + pos_all[:, 1]
    picked = sources[:, None] == jnp.arange(SOURCES)[None, :]
    pos_all = jnp.sum(jnp.where(picked[:, :, None], pos_all[None], 0), 1)
    kpos = pos_all.reshape(SOURCES, NSTEPS, KSTEP).transpose(1, 0, 2)
    first_pos = jnp.min(kpos, (1, 2))
    last_pos = jnp.max(kpos, (1, 2))
    kpos = kpos.reshape(NSTEPS, 1, KEYS)
    by_block = sorted_pos.reshape(BLOCKS, BLOCK)
    full = jnp.sum((last_pos[None, :] <= by_block[:, :1]).astype(jnp.int32), 1)
    need = jnp.sum((first_pos[None, :] <= by_block[:, -1:]).astype(jnp.int32), 1)
    bounds = jnp.stack([full, need])
    qpos = jnp.tile(by_block[:, None, :], (1, HEADS, 1)).reshape(BLOCKS, HEADS * BLOCK, 1)

    swap = [
        ((a * 2 + c) * 8 + b, (b * 2 + c) * 8 + a)
        for a in range(8)
        for c in range(2)
        for b in range(8)
    ]
    moved = lax.ppermute(w_out, SEQ + TENSOR, swap)
    moved, other_kv = lax.optimization_barrier((moved, other_kv))
    w_out_all = lax.all_gather(moved, SEQ, axis=0, tiled=True).reshape(SOURCES, 512, 512)

    mix_ids = jnp.stack([z * 4 + (x + d) % 4 for z in (zh, 1 - zh) for d in (0, 3, 1, 2)])
    base = tokens
    contexts = []
    for first, count in CALLS:
        at = slice(first, first + count)
        own = attend(bounds[:, at], queries, qpos, own_kv, other_kv, kpos, first, count)
        contexts.append(own)
        across = lax.ppermute(own, "zh", SWAP)
        near = [own] + [lax.ppermute(own, "x", s) for s in (NEXT, PREV, ACROSS)]
        far = [across] + [lax.ppermute(across, "x", s) for s in (NEXT, PREV)]
        found = near + far + [lax.ppermute(near[3], "zh", SWAP)]
        last = first + count == BLOCKS
        rows = slice(first * BLOCK, (first + count) * BLOCK)
        base = mix(found, mix_ids.astype(jnp.int32), w_out_all, back[:, rows], base, last)
    context = jnp.dot(back, jnp.concatenate(contexts, 0), preferred_element_type=f32).astype(bf16)
    return (base, context)


def solution(mesh):
    fine = Mesh(mesh.devices.reshape(4, 2, 2, 2, 4), SEQ + TENSOR)
    in_specs = (
        P(SEQ, TENSOR),
        P(SEQ),
        P(),
        P(SEQ, TENSOR),
        P(SEQ, TENSOR),
        P(SEQ, TENSOR),
        P(TENSOR),
        P(TENSOR),
        P(TENSOR),
        P(TENSOR, SEQ),
    )
    out_specs = (P(SEQ, TENSOR), P(SEQ, TENSOR))
    return jax.shard_map(block, mesh=fine, in_specs=in_specs, out_specs=out_specs, check_vma=False)
```

```python
import math

import jax
import jax.numpy as jnp
from jax import lax
from jax.experimental import pallas as pl
from jax.experimental.pallas import tpu as pltpu
from jax.sharding import Mesh, PartitionSpec as P


HD = 128
NORM_EPS = 1e-06
ROPE_BASE = 1000000.0
NEG_FILL = -1e30
SEQ = ("y", "zl", "core")
TENSOR = ("zh", "x")
ROWS = 512
FEAT = 1024
MODEL = 8192
SOURCES = 16
GROUPS = 8
HEADS = 4
POS_ROWS = 16
KSTEP = 64
NSTEPS = ROWS // KSTEP
KEYS = SOURCES * KSTEP
BLOCK = 128
BLOCKS = ROWS // BLOCK
CALLS = ((0, 2), (2, 2))
PER_STEP = 2
QSCALE = HD**-0.5 * math.log2(math.e)


NEXT = [(i, (i + 1) % 4) for i in range(4)]
PREV = [(i, (i - 1) % 4) for i in range(4)]
ACROSS = [(i, (i + 2) % 4) for i in range(4)]
SWAP = [(0, 1), (1, 0)]


def fetch_all(pieces, slots, buffer, sems, step):
    def fetch(i):
        slot, start, size = slots[i]
        return pltpu.make_async_copy(pieces[i], buffer.at[slot, pl.ds(start, size)], sems.at[i])

    @pl.when(step == 0)
    def _():
        for i in range(len(slots)):
            fetch(i).start()

    for k in range(buffer.shape[0] // PER_STEP):

        @pl.when(step == k)
        def _(k=k):
            for i, (slot, _, _) in enumerate(slots):
                if slot // PER_STEP == k:
                    fetch(i).wait()


def whole(*shape):
    return pl.BlockSpec(shape, lambda k, ids: (0,) * len(shape))


def project_body(slots, steps, queries, partial, ids, *refs):
    pieces = refs[: len(slots)]
    refs = refs[len(slots) :]
    w_refs = refs[:PER_STEP]
    refs = refs[PER_STEP:]
    step = pl.program_id(0)
    if partial == "first":
        acc, tbuf, sems = refs
    elif partial == "last":
        before_ref, inverse_ref, bias_ref, cos_ref, sin_ref, out_ref, tbuf, acc, sems = refs
    else:
        inverse_ref, bias_ref, cos_ref, sin_ref, out_ref, tbuf, acc, sems = refs
    fetch_all(pieces, slots, tbuf, sems, step)
    half = FEAT // 2
    total = None
    for i in range(PER_STEP):
        rows = tbuf[step * PER_STEP + i]
        for j in range(2):
            part = jnp.dot(
                rows[:, j * half : (j + 1) * half], w_refs[i][j], preferred_element_type=jnp.float32
            )
            total = part if total is None else total + part

    @pl.when(step == 0)
    def _():
        acc[...] = total if partial != "last" else total + before_ref[...]

    @pl.when(step > 0)
    def _():
        acc[...] += total

    if partial == "first":
        return

    @pl.when(step == steps - 1)
    def _():
        inverse = inverse_ref[...]
        cosine = cos_ref[...]
        sines = sin_ref[...]

        def head(i):
            return acc[:, i * HD : (i + 1) * HD] * inverse + bias_ref[:, i * HD : (i + 1) * HD]

        def turned(u):
            return u * cosine + pltpu.roll(u, HD // 2, 1) * sines

        if queries:
            for i in range(HEADS):
                q = (turned(head(i)) * QSCALE).astype(jnp.bfloat16)
                for b in range(BLOCKS):
                    out_ref[b, i * BLOCK : (i + 1) * BLOCK] = q[b * BLOCK : (b + 1) * BLOCK]
        else:
            out_ref[:, :HD] = turned(head(0)).astype(jnp.bfloat16)
            out_ref[:, HD:] = head(1).astype(jnp.bfloat16)


def w_spec(i, width, first=0):
    def at(k, ids):
        group = (k + first) * PER_STEP + i
        return (ids[0, group], 0, ids[1, group], 0, 0)

    return pl.BlockSpec((None, 2, None, ROWS, width), at)


def project(pieces, slots, ids, weights, finish, queries, partial=None, before=None):
    width = HEADS * HD if queries else 2 * HD
    groups = GROUPS if partial is None else GROUPS // 2
    first = groups // PER_STEP if partial == "last" else 0
    steps = groups // PER_STEP
    dtype = jnp.bfloat16
    if partial == "first":
        out_shape, dtype = ((ROWS, width), jnp.float32)
        extra, extra_specs = ((), [])
    else:
        out_shape = (BLOCKS, HEADS * BLOCK, HD) if queries else (ROWS, 2 * HD)
        extra = finish if before is None else (before,) + finish
        extra_specs = [] if before is None else [whole(ROWS, width)]
        extra_specs += [whole(ROWS, 1), whole(1, width), whole(ROWS, HD), whole(ROWS, HD)]
    scratch = [pltpu.VMEM((groups, ROWS, FEAT), jnp.bfloat16)]
    if partial != "first":
        scratch += [pltpu.VMEM((ROWS, width), jnp.float32)]
    scratch += [pltpu.SemaphoreType.DMA((len(pieces),))]

    def body(*refs):
        project_body(slots, steps, queries, partial, *refs)

    return pl.pallas_call(
        body,
        grid_spec=pltpu.PrefetchScalarGridSpec(
            num_scalar_prefetch=1,
            grid=(steps,),
            in_specs=[pl.BlockSpec(memory_space=pl.ANY)] * len(pieces)
            + [w_spec(i, width, first) for i in range(PER_STEP)]
            + extra_specs,
            out_specs=whole(*out_shape),
            scratch_shapes=scratch,
        ),
        out_shape=jax.ShapeDtypeStruct(out_shape, dtype),
        compiler_params=pltpu.CompilerParams(dimension_semantics=("arbitrary",)),
        cost_estimate=pl.CostEstimate(
            flops=2 * ROWS * groups * FEAT * width, transcendentals=0, bytes_accessed=16 << 20
        ),
    )(ids, *pieces, *([weights] * PER_STEP), *extra)


def attend_body(bounds, q_ref, qpos_ref, own_ref, other_ref, kpos_ref, out_ref, kv_ref, top, acc, sems):
    block_at = pl.program_id(0)
    full = bounds[0, block_at]
    need = bounds[1, block_at]

    def fetch(i):
        source = (own_ref, other_ref)[i]
        half = SOURCES // 2
        return pltpu.make_async_copy(source, kv_ref.at[pl.ds(i * half, half)], sems.at[i])

    @pl.when(block_at == 0)
    def _():
        fetch(0).start()
        fetch(1).start()

    top[...] = jnp.full_like(top, NEG_FILL)
    acc[...] = jnp.zeros_like(acc)

    @pl.when(block_at == 0)
    def _():
        fetch(0).wait()
        fetch(1).wait()

    ones = jnp.ones((KEYS, HD), jnp.bfloat16)
    parts = top.shape[0]
    rows = top.shape[1]

    def one_step(j, masked):
        at = pl.multiple_of(j * KSTEP, KSTEP)
        block = kv_ref[:, pl.ds(at, KSTEP), :].reshape(KEYS, 2 * HD)
        keys = block[:, :HD]
        values = jnp.concatenate([block[:, HD:], ones], axis=1)

        def scores_of(h):
            return lax.dot_general(
                q_ref[0, h * rows : (h + 1) * rows],
                keys,
                (((1,), (1,)), ((), ())),
                preferred_element_type=jnp.float32,
            )

        following = scores_of(0)
        for h in range(parts):
            scores = following
            following = scores_of(h + 1) if h + 1 < parts else None
            if masked:
                allowed = kpos_ref[j] <= qpos_ref[0, h * rows : (h + 1) * rows]
                scores = jnp.where(allowed, scores, NEG_FILL)
            old = top[h]
            new = jnp.maximum(old, jnp.max(scores, axis=1, keepdims=True))
            weights = jnp.exp2(scores - jnp.concatenate([new] * (KEYS // HD), axis=1))
            rescale = jnp.exp2(old - new)
            top[h] = new
            acc[h] = acc[h] * jnp.concatenate([rescale, rescale], axis=1) + jnp.dot(
                weights.astype(jnp.bfloat16), values, preferred_element_type=jnp.float32
            )

    def unmasked(j, carry):
        one_step(j, False)
        return carry

    def masked(j, carry):
        one_step(j, True)
        return carry

    lax.fori_loop(0, full, unmasked, 0)
    lax.fori_loop(full, need, masked, 0)
    for h in range(HEADS):
        part, at = (h * BLOCK // rows, h * BLOCK % rows)
        done = acc[part, at : at + BLOCK, :HD] / acc[part, at : at + BLOCK, HD:]
        out_ref[:, h * HD : (h + 1) * HD] = done.astype(jnp.bfloat16)


def attend(bounds, queries, qpos, own, other, kpos, first, count):
    part = 2 * BLOCK
    return pl.pallas_call(
        attend_body,
        grid_spec=pltpu.PrefetchScalarGridSpec(
            num_scalar_prefetch=1,
            grid=(count,),
            in_specs=[
                pl.BlockSpec((1, HEADS * BLOCK, HD), lambda c, b: (c + first, 0, 0)),
                pl.BlockSpec((1, HEADS * BLOCK, 1), lambda c, b: (c + first, 0, 0)),
                pl.BlockSpec(memory_space=pl.ANY),
                pl.BlockSpec(memory_space=pl.ANY),
                whole(NSTEPS, 1, KEYS),
            ],
            out_specs=pl.BlockSpec((BLOCK, HEADS * HD), lambda c, b: (c, 0)),
            scratch_shapes=[
                pltpu.VMEM((SOURCES, ROWS, 2 * HD), jnp.bfloat16),
                pltpu.VMEM((HEADS * BLOCK // part, part, HD), jnp.float32),
                pltpu.VMEM((HEADS * BLOCK // part, part, 2 * HD), jnp.float32),
                pltpu.SemaphoreType.DMA((2,)),
            ],
        ),
        out_shape=jax.ShapeDtypeStruct((BLOCK * count, HEADS * HD), jnp.bfloat16),
        compiler_params=pltpu.CompilerParams(dimension_semantics=("arbitrary",)),
        cost_estimate=pl.CostEstimate(
            flops=4 * HEADS * BLOCK * count * SOURCES * ROWS * HD,
            transcendentals=HEADS * BLOCK * count * SOURCES * ROWS,
            bytes_accessed=6 << 20,
        ),
    )(bounds, queries, qpos, own, other, kpos)


def mix_body(slots, ids, *refs):
    pieces = refs[: len(slots)]
    refs = refs[len(slots) :]
    w_refs = refs[:PER_STEP]
    back_ref, base_ref, out_ref, cbuf, acc, sems = refs[PER_STEP:]
    step = pl.program_id(0)
    fetch_all(pieces, slots, cbuf, sems, step)
    parts = []
    for half in range(2):
        total = None
        for i in range(PER_STEP):
            part = jnp.dot(
                cbuf[step * PER_STEP + i], w_refs[i][half], preferred_element_type=jnp.float32
            )
            total = part if total is None else total + part
        parts.append(total)

    @pl.when(step == 0)
    def _():
        for half in range(2):
            acc[:, half * 512 : (half + 1) * 512] = parts[half]

    @pl.when(step > 0)
    def _():
        for half in range(2):
            acc[:, half * 512 : (half + 1) * 512] += parts[half]

    @pl.when(step == GROUPS // PER_STEP - 1)
    def _():
        back = back_ref[...]
        high = acc[...].astype(jnp.bfloat16)
        low = (acc[...] - high.astype(jnp.float32)).astype(jnp.bfloat16)
        mixed = jnp.dot(back, high, preferred_element_type=jnp.float32) + jnp.dot(
            back, low, preferred_element_type=jnp.float32
        )
        out_ref[...] = (base_ref[...].astype(jnp.float32) + mixed).astype(out_ref.dtype)


def mix(pieces, ids, w_out, back, base, last):
    rows = pieces[0].shape[0]
    slots = [(i, 0, rows) for i in range(GROUPS)]

    def body(*refs):
        mix_body(slots, *refs)

    return pl.pallas_call(
        body,
        grid_spec=pltpu.PrefetchScalarGridSpec(
            num_scalar_prefetch=1,
            grid=(GROUPS // PER_STEP,),
            in_specs=[pl.BlockSpec(memory_space=pl.ANY)] * len(pieces)
            + [w_spec(i, 512) for i in range(PER_STEP)]
            + [whole(ROWS, rows), whole(ROWS, FEAT)],
            out_specs=whole(ROWS, FEAT),
            scratch_shapes=[
                pltpu.VMEM((GROUPS, rows, HEADS * HD), jnp.bfloat16),
                pltpu.VMEM((rows, FEAT), jnp.float32),
                pltpu.SemaphoreType.DMA((len(pieces),)),
            ],
        ),
        out_shape=jax.ShapeDtypeStruct((ROWS, FEAT), jnp.bfloat16 if last else jnp.float32),
        compiler_params=pltpu.CompilerParams(dimension_semantics=("arbitrary",)),
        cost_estimate=pl.CostEstimate(
            flops=2 * rows * HEADS * HD * GROUPS * FEAT, transcendentals=0, bytes_accessed=12 << 20
        ),
        name="mix_last" if last else "mix_first",
    )(ids, *pieces, *([w_out] * PER_STEP), back, base)


def block(tokens, positions, norm_gain, w_query, w_key, w_value, b_query, b_key, b_value, w_out):
    bf16, f32 = (jnp.bfloat16, jnp.float32)
    seq_at = lax.axis_index(SEQ)
    zh, x = (lax.axis_index("zh"), lax.axis_index("x"))

    rank = jnp.sum((positions[None, :] < positions[:, None]).astype(jnp.int32), 1)
    chosen = rank[None, :] == jnp.arange(ROWS, dtype=jnp.int32)[:, None]
    order = chosen.astype(bf16)
    back = (rank[:, None] == jnp.arange(ROWS, dtype=jnp.int32)[None, :]).astype(bf16)
    sorted_pos = jnp.sum(jnp.where(chosen, positions[None, :], 0), 1)
    sorted_tokens = jnp.dot(order, tokens, preferred_element_type=f32).astype(bf16)

    gain = lax.dynamic_slice(norm_gain, (seq_at * ROWS,), (ROWS,))[:, None]
    w_kv = (jnp.concatenate((w_key, w_value), 1).astype(f32) * gain).astype(bf16)
    w_q = (w_query.astype(f32) * gain).astype(bf16)
    pos_rows = jnp.stack([sorted_pos >> 7, sorted_pos & 127]).astype(bf16)
    pos_rows = jnp.pad(pos_rows.reshape(4, 2 * HD), ((0, POS_ROWS - 4), (0, 0)))
    w_kv = jnp.concatenate([w_kv, pos_rows], 0)

    def over_seq(own, flip):
        both = jnp.concatenate([own, flip], 0)
        whole_seq = lax.all_gather(both, ("y", "core"), axis=0, tiled=True)
        return whole_seq.reshape((4, 2, 2) + own.shape)

    kv_flip = lax.ppermute(w_kv, "zl", SWAP)
    q_flip = lax.ppermute(w_q, "zl", SWAP)
    w_kv_all = over_seq(w_kv, kv_flip)
    w_q_all = over_seq(w_q, q_flip)

    def ring(own):
        half = own.shape[0] // 2
        left = lax.ppermute(own, "x", NEXT)
        right = lax.ppermute(own, "x", PREV)
        low, high = (left[:half], right[half:])
        low = lax.ppermute(low, "x", NEXT)
        high = lax.ppermute(high, "x", PREV)
        return left, right, low, high

    other = lax.ppermute(sorted_tokens, "zh", SWAP)
    left, right, low, high = ring(sorted_tokens)
    oleft = lax.ppermute(other, "x", NEXT)
    oright = lax.ppermute(other, "x", PREV)
    olow = lax.ppermute(low, "zh", SWAP)
    ohigh = lax.ppermute(high, "zh", SWAP)

    def square(piece):
        wide = piece.astype(f32)
        return jnp.sum(wide * wide, 1, keepdims=True)

    total = sum(square(p) for p in (sorted_tokens, left, right, other, oleft, oright))
    total += jnp.concatenate([square(low), square(high)], 0)
    total += jnp.concatenate([square(olow), square(ohigh)], 0)
    inverse = lax.rsqrt(total * (1.0 / MODEL) + NORM_EPS)
    y, zl, core = (lax.axis_index("y"), lax.axis_index("zl"), lax.axis_index("core"))
    groups = jnp.stack([z * 4 + (x + d) % 4 for z in (zh, 1 - zh) for d in (0, 3, 1, 2)])
    ids = jnp.stack([groups // 2, (groups % 2) ^ zl]).astype(jnp.int32)
    half = ROWS // 2
    pieces = [sorted_tokens, left, right, low, high, other, oleft, oright, olow, ohigh]
    slots = [(0, 0, ROWS), (1, 0, ROWS), (2, 0, ROWS), (3, 0, half), (3, half, half)]

    half_dim = HD // 2
    inv_freq = ROPE_BASE ** (-jnp.arange(half_dim, dtype=f32) * 2.0 / HD)
    angles = sorted_pos.astype(f32)[:, None] * inv_freq[None, :]
    cosine = jnp.cos(angles)
    sines = jnp.sin(angles)
    cosine = jnp.concatenate([cosine, cosine], 1)
    sines = jnp.concatenate([-sines, sines], 1)

    chips = [(y, 0), (y, 1)] + [((y + d) % 4, f) for f in (0, 1) for d in (3, 1, 2)]
    sources = jnp.stack([(a * 2 + c) * 2 + f for c in (core, 1 - core) for a, f in chips])
    pos_all = w_kv_all[:, :, :, ROWS : ROWS + 4].astype(jnp.int32).reshape(SOURCES, 2, ROWS)
    pos_all = pos_all[:, 0] * 128 + pos_all[:, 1]
    picked = sources[:, None] == jnp.arange(SOURCES)[None, :]
    pos_all = jnp.sum(jnp.where(picked[:, :, None], pos_all[None], 0), 1)
    kpos = pos_all.reshape(SOURCES, NSTEPS, KSTEP).transpose(1, 0, 2)
    first_pos = jnp.min(kpos, (1, 2))
    last_pos = jnp.max(kpos, (1, 2))
    kpos = kpos.reshape(NSTEPS, 1, KEYS)
    by_block = sorted_pos.reshape(BLOCKS, BLOCK)
    full = jnp.sum((last_pos[None, :] <= by_block[:, :1]).astype(jnp.int32), 1)
    need = jnp.sum((first_pos[None, :] <= by_block[:, -1:]).astype(jnp.int32), 1)
    bounds = jnp.stack([full, need])
    qpos = jnp.tile(by_block[:, None, :], (1, HEADS, 1)).reshape(BLOCKS, HEADS * BLOCK, 1)

    kv_bias = jnp.concatenate((b_key, b_value))[None, :]
    start = project(pieces[:5], slots, ids, w_kv_all, (), False, "first")
    inverse, kpos, bounds, qpos, start = lax.optimization_barrier(
        (inverse, kpos, bounds, qpos, start)
    )
    finish = (inverse, kv_bias, cosine, sines)
    kv = project(pieces[5:], slots, ids, w_kv_all, finish, False, "last", start)

    def flipped(steps):
        turn = dict(steps)
        return [(a * 2 + b, turn[a] * 2 + 1 - b) for a in range(4) for b in range(2)]

    found = [kv, lax.ppermute(kv, "zl", SWAP)]
    found += [lax.ppermute(kv, "y", steps) for steps in (NEXT, PREV, ACROSS)]
    found += [lax.ppermute(kv, ("y", "zl"), flipped(steps)) for steps in (NEXT, PREV, ACROSS)]
    own_kv = jnp.stack(found)
    other_kv = lax.ppermute(own_kv, "core", SWAP)

    finish = (inverse, b_query[None, :], cosine, sines)
    both_slots = slots + [(slot + 4, at, size) for slot, at, size in slots]
    queries = project(pieces, both_slots, ids, w_q_all, finish, True)

    def homes(flip):
        return [
            ((a * 2 + c) * 8 + b, ((b ^ flip) * 2 + c) * 8 + a)
            for a in range(8)
            for c in range(2)
            for b in range(8)
        ]

    moved = lax.ppermute(w_out, SEQ + TENSOR, homes(0))
    moved_flip = lax.ppermute(w_out, SEQ + TENSOR, homes(1))
    w_out_all = over_seq(moved, moved_flip)

    base = tokens
    contexts = []
    for first, count in CALLS:
        at = slice(first, first + count)
        own = attend(bounds[:, at], queries, qpos, own_kv, other_kv, kpos, first, count)
        contexts.append(own)
        across = lax.ppermute(own, "zh", SWAP)
        near = [own] + [lax.ppermute(own, "x", s) for s in (NEXT, PREV, ACROSS)]
        far = [across] + [lax.ppermute(across, "x", s) for s in (NEXT, PREV)]
        found = near + far + [lax.ppermute(near[3], "zh", SWAP)]
        last = first + count == BLOCKS
        rows = slice(first * BLOCK, (first + count) * BLOCK)
        base = mix(found, ids, w_out_all, back[:, rows], base, last)
    context = jnp.dot(back, jnp.concatenate(contexts, 0), preferred_element_type=f32).astype(bf16)
    return (base, context)


def solution(mesh):
    fine = Mesh(mesh.devices.reshape(4, 2, 2, 2, 4), SEQ + TENSOR)
    in_specs = (
        P(SEQ, TENSOR),
        P(SEQ),
        P(),
        P(SEQ, TENSOR),
        P(SEQ, TENSOR),
        P(SEQ, TENSOR),
        P(TENSOR),
        P(TENSOR),
        P(TENSOR),
        P(TENSOR, SEQ),
    )
    out_specs = (P(SEQ, TENSOR), P(SEQ, TENSOR))
    return jax.shard_map(block, mesh=fine, in_specs=in_specs, out_specs=out_specs, check_vma=False)
```

```python
import math

import jax
import jax.numpy as jnp
from jax import lax
from jax.experimental import pallas as pl
from jax.experimental.pallas import tpu as pltpu
from jax.sharding import Mesh, PartitionSpec as P


HD = 128
NORM_EPS = 1e-06
ROPE_BASE = 1000000.0
NEG_FILL = -1e30
SEQ = ("y", "zl", "core")
TENSOR = ("zh", "x")
ROWS = 512
FEAT = 1024
MODEL = 8192
SOURCES = 16
GROUPS = 8
HEADS = 4
POS_ROWS = 16
KSTEP = 64
NSTEPS = ROWS // KSTEP
KEYS = SOURCES * KSTEP
BLOCK = 128
BLOCKS = ROWS // BLOCK
CALLS = ((0, 2), (2, 2))
PER_DOT = 1
QSCALE = HD**-0.5 * math.log2(math.e)


IN_ORDER = ("arbitrary",)
FIRST, LAST = (1, 2)
NEXT = [(i, (i + 1) % 4) for i in range(4)]
PREV = [(i, (i - 1) % 4) for i in range(4)]
ACROSS = [(i, (i + 2) % 4) for i in range(4)]
SWAP = [(0, 1), (1, 0)]


def whole(*shape):
    return pl.BlockSpec(shape, lambda k, ids: (0,) * len(shape))


def dots(ids, pieces, slots, w_ref, w_to, size, buffer, w_buffer, acc, sems, before=None):
    groups = buffer.shape[1] // size
    made = []
    for i, (slot, start, count) in enumerate(slots):
        to = buffer.at[pl.ds(start, count), pl.ds(slot * size, size)]
        made.append((slot, pltpu.make_async_copy(pieces[i], to, sems.at[i])))
    for g in range(groups):
        for c in range(2):
            source = w_ref.at[ids[0, g], c, ids[1, g], pl.ds(0, ROWS)]
            sem = sems.at[len(slots) + g * 2 + c]
            made.append((g, pltpu.make_async_copy(source, w_to(w_buffer, g, c), sem)))
    made.sort(key=lambda pair: pair[0])
    for _, copy in made:
        copy.start()
    for k in range(groups // PER_DOT):
        for slot, copy in made:
            if slot // PER_DOT == k:
                copy.wait()
        deep = slice(k * PER_DOT * size, (k + 1) * PER_DOT * size)
        part = jnp.dot(buffer[:, deep], w_buffer[deep, :], preferred_element_type=jnp.float32)
        if k == 0:
            acc[...] = part if before is None else part + before[...]
        else:
            acc[...] += part


def rows_to(w_buffer, g, c):
    return w_buffer.at[pl.ds((g * 2 + c) * ROWS, ROWS)]


def columns_to(w_buffer, g, c):
    return w_buffer.at[pl.ds(g * ROWS, ROWS), pl.ds(c * ROWS, ROWS)]


def project_body(slots, queries, partial, ids, *refs):
    pieces = refs[: len(slots)]
    w_ref = refs[len(slots)]
    refs = refs[len(slots) + 1 :]
    before = None
    if partial == FIRST:
        acc, buffer, w_buffer, sems = refs
    else:
        if partial == LAST:
            before, refs = (refs[0], refs[1:])
        inverse_ref, bias_ref, cos_ref, sin_ref, out_ref, buffer, w_buffer, acc, sems = refs
    dots(ids, pieces, slots, w_ref, rows_to, FEAT, buffer, w_buffer, acc, sems, before)
    if partial == FIRST:
        return
    inverse = inverse_ref[...]
    cosine = cos_ref[...]
    sines = sin_ref[...]

    def head(i):
        return acc[:, i * HD : (i + 1) * HD] * inverse + bias_ref[:, i * HD : (i + 1) * HD]

    def turned(u):
        return u * cosine + pltpu.roll(u, HD // 2, 1) * sines

    if queries:
        for i in range(HEADS):
            q = (turned(head(i)) * QSCALE).astype(jnp.bfloat16)
            for b in range(BLOCKS):
                out_ref[b, i * BLOCK : (i + 1) * BLOCK] = q[b * BLOCK : (b + 1) * BLOCK]
    else:
        out_ref[:, :HD] = turned(head(0)).astype(jnp.bfloat16)
        out_ref[:, HD:] = head(1).astype(jnp.bfloat16)


SCALARS = pl.BlockSpec(memory_space=pltpu.SMEM)
ANYWHERE = pl.BlockSpec(memory_space=pl.ANY)
NEAR = pl.BlockSpec(memory_space=pltpu.VMEM)


def project(pieces, slots, ids, weights, finish, queries, partial=None, before=None):
    width = HEADS * HD if queries else 2 * HD
    groups = GROUPS if partial is None else GROUPS // 2
    ids = ids[:, GROUPS - groups :] if partial == LAST else ids[:, :groups]
    dtype = jnp.bfloat16
    out_shape = (BLOCKS, HEADS * BLOCK, HD) if queries else (ROWS, 2 * HD)
    extra = finish if before is None else (before,) + finish
    scratch = [
        pltpu.VMEM((ROWS, groups * FEAT), jnp.bfloat16),
        pltpu.VMEM((groups * FEAT, width), jnp.bfloat16),
    ]
    if partial == FIRST:
        out_shape, dtype = ((ROWS, width), jnp.float32)
    else:
        scratch += [pltpu.VMEM((ROWS, width), jnp.float32)]
    scratch += [pltpu.SemaphoreType.DMA((len(pieces) + 2 * groups,))]

    def body(*refs):
        project_body(slots, queries, partial, *refs)

    return pl.pallas_call(
        body,
        in_specs=[SCALARS] + [ANYWHERE] * (len(pieces) + 1) + [NEAR] * len(extra),
        out_specs=NEAR,
        scratch_shapes=scratch,
        out_shape=jax.ShapeDtypeStruct(out_shape, dtype),
        cost_estimate=pl.CostEstimate(
            flops=2 * ROWS * groups * FEAT * width, transcendentals=0, bytes_accessed=16 << 20
        ),
        name="pq" if queries else ("pk0" if partial == FIRST else "pk1"),
    )(ids, *pieces, weights, *extra)


def attend_body(first, bounds, q_ref, qpos_ref, kpos_ref, *refs):
    pairs = refs[: SOURCES // 2]
    out_ref, kv_ref, top, acc, sems = refs[SOURCES // 2 :]
    block_at = pl.program_id(0)
    full = bounds[0, block_at]
    need = bounds[1, block_at]

    def fetch(i):
        return pltpu.make_async_copy(pairs[i], kv_ref.at[pl.ds(2 * i, 2)], sems.at[i])

    @pl.when(block_at == 0)
    def _():
        for i in range(len(pairs)):
            fetch(i).start()

    top[...] = jnp.full_like(top, NEG_FILL)
    acc[...] = jnp.zeros_like(acc)

    @pl.when(block_at == 0)
    def _():
        for i in range(len(pairs)):
            fetch(i).wait()

    ones = jnp.ones((KEYS, HD), jnp.bfloat16)
    parts = top.shape[0]
    rows = top.shape[1]

    def one_step(j, masked):
        at = pl.multiple_of(j * KSTEP, KSTEP)
        block = kv_ref[:, pl.ds(at, KSTEP), :].reshape(KEYS, 2 * HD)
        keys = block[:, :HD]
        values = jnp.concatenate([block[:, HD:], ones], axis=1)

        def scores_of(h):
            return lax.dot_general(
                q_ref[0, h * rows : (h + 1) * rows],
                keys,
                (((1,), (1,)), ((), ())),
                preferred_element_type=jnp.float32,
            )

        following = scores_of(0)
        for h in range(parts):
            scores = following
            following = scores_of(h + 1) if h + 1 < parts else None
            if masked:
                allowed = kpos_ref[j] <= qpos_ref[0, h * rows : (h + 1) * rows]
                scores = jnp.where(allowed, scores, NEG_FILL)
            old = top[h]
            new = jnp.maximum(old, jnp.max(scores, axis=1, keepdims=True))
            weights = jnp.exp2(scores - jnp.concatenate([new] * (KEYS // HD), axis=1))
            rescale = jnp.exp2(old - new)
            top[h] = new
            acc[h] = acc[h] * jnp.concatenate([rescale, rescale], axis=1) + jnp.dot(
                weights.astype(jnp.bfloat16), values, preferred_element_type=jnp.float32
            )

    def unmasked(j, carry):
        one_step(j, False)
        return carry

    def masked(j, carry):
        one_step(j, True)
        return carry

    if first == 0:
        lax.fori_loop(0, need, masked, 0)
    else:
        lax.fori_loop(0, full, unmasked, 0)
        lax.fori_loop(full, need, masked, 0)
    for h in range(HEADS):
        part, at = (h * BLOCK // rows, h * BLOCK % rows)
        done = acc[part, at : at + BLOCK, :HD] / acc[part, at : at + BLOCK, HD:]
        out_ref[:, h * HD : (h + 1) * HD] = done.astype(jnp.bfloat16)


def attend(bounds, queries, qpos, pairs, kpos, first, count):
    part = 2 * BLOCK

    def body(*refs):
        attend_body(first, *refs)

    return pl.pallas_call(
        body,
        grid_spec=pltpu.PrefetchScalarGridSpec(
            num_scalar_prefetch=1,
            grid=(count,),
            in_specs=[
                pl.BlockSpec((1, HEADS * BLOCK, HD), lambda c, b: (c + first, 0, 0)),
                pl.BlockSpec((1, HEADS * BLOCK, 1), lambda c, b: (c + first, 0, 0)),
                whole(NSTEPS, 1, KEYS),
            ]
            + [pl.BlockSpec(memory_space=pl.ANY)] * len(pairs),
            out_specs=pl.BlockSpec((BLOCK, HEADS * HD), lambda c, b: (c, 0)),
            scratch_shapes=[
                pltpu.VMEM((SOURCES, ROWS, 2 * HD), jnp.bfloat16),
                pltpu.VMEM((HEADS * BLOCK // part, part, HD), jnp.float32),
                pltpu.VMEM((HEADS * BLOCK // part, part, 2 * HD), jnp.float32),
                pltpu.SemaphoreType.DMA((len(pairs),)),
            ],
        ),
        out_shape=jax.ShapeDtypeStruct((BLOCK * count, HEADS * HD), jnp.bfloat16),
        compiler_params=pltpu.CompilerParams(dimension_semantics=IN_ORDER),
        cost_estimate=pl.CostEstimate(
            flops=4 * HEADS * BLOCK * count * SOURCES * ROWS * HD,
            transcendentals=HEADS * BLOCK * count * SOURCES * ROWS,
            bytes_accessed=6 << 20,
        ),
    )(bounds, queries, qpos, kpos, *pairs)


def mix_body(slots, ids, *refs):
    pieces = refs[: len(slots)]
    w_ref, back_ref, base_ref, out_ref, buffer, w_buffer, acc, sems = refs[len(slots) :]
    dots(ids, pieces, slots, w_ref, columns_to, ROWS, buffer, w_buffer, acc, sems)
    back = back_ref[...]
    high = acc[...].astype(jnp.bfloat16)
    low = (acc[...] - high.astype(jnp.float32)).astype(jnp.bfloat16)
    mixed = jnp.dot(back, high, preferred_element_type=jnp.float32) + jnp.dot(
        back, low, preferred_element_type=jnp.float32
    )
    out_ref[...] = (base_ref[...].astype(jnp.float32) + mixed).astype(out_ref.dtype)


def mix(pieces, ids, w_out, back, base, last):
    rows = pieces[0].shape[0]
    slots = [(i, 0, rows) for i in range(GROUPS)]

    def body(*refs):
        mix_body(slots, *refs)

    return pl.pallas_call(
        body,
        in_specs=[SCALARS] + [ANYWHERE] * (len(pieces) + 1) + [NEAR] * 2,
        out_specs=NEAR,
        scratch_shapes=[
            pltpu.VMEM((rows, GROUPS * ROWS), jnp.bfloat16),
            pltpu.VMEM((GROUPS * ROWS, FEAT), jnp.bfloat16),
            pltpu.VMEM((rows, FEAT), jnp.float32),
            pltpu.SemaphoreType.DMA((len(pieces) + 2 * GROUPS,)),
        ],
        out_shape=jax.ShapeDtypeStruct((ROWS, FEAT), jnp.bfloat16 if last else jnp.float32),
        cost_estimate=pl.CostEstimate(
            flops=2 * rows * HEADS * HD * GROUPS * FEAT, transcendentals=0, bytes_accessed=12 << 20
        ),
        name="m1" if last else "m0",
    )(ids, *pieces, w_out, back, base)


def block(tokens, positions, norm_gain, w_query, w_key, w_value, b_query, b_key, b_value, w_out):
    bf16, f32 = (jnp.bfloat16, jnp.float32)
    seq_at = lax.axis_index(SEQ)
    zh, x = (lax.axis_index("zh"), lax.axis_index("x"))

    spread = [
        (
            ((yy * 2 + zz) * 2 + hh) * 4 + xx,
            ((((yy % 2) * 2 + zz + xx) % 4 * 2 + hh) * 2 + yy // 2) * 4 + xx,
        )
        for yy in range(4)
        for zz in range(2)
        for hh in range(2)
        for xx in range(4)
    ]
    moved = lax.ppermute(w_out, ("y", "zl", "zh", "x"), spread)

    rank = jnp.sum((positions[None, :] < positions[:, None]).astype(jnp.int32), 1)
    chosen = rank[None, :] == jnp.arange(ROWS, dtype=jnp.int32)[:, None]
    order = chosen.astype(bf16)
    back = (rank[:, None] == jnp.arange(ROWS, dtype=jnp.int32)[None, :]).astype(bf16)
    sorted_pos = jnp.sum(jnp.where(chosen, positions[None, :], 0), 1)
    sorted_tokens = jnp.dot(order, tokens, preferred_element_type=f32).astype(bf16)

    gain = lax.dynamic_slice(norm_gain, (seq_at * ROWS,), (ROWS,))[:, None]
    w_kv = (jnp.concatenate((w_key, w_value), 1).astype(f32) * gain).astype(bf16)
    w_q = (w_query.astype(f32) * gain).astype(bf16)
    pos_rows = jnp.stack([sorted_pos >> 7, sorted_pos & 127]).astype(bf16)
    pos_rows = jnp.pad(pos_rows.reshape(4, 2 * HD), ((0, POS_ROWS - 4), (0, 0)))
    w_kv = jnp.concatenate([w_kv, pos_rows], 0)

    def over_seq(own, flip):
        both = jnp.concatenate([own, flip], 0)
        whole_seq = lax.all_gather(both, ("y", "core"), axis=0, tiled=True)
        return whole_seq.reshape((4, 2, 2) + own.shape)

    kv_flip = lax.ppermute(w_kv, "zl", SWAP)
    q_flip = lax.ppermute(w_q, "zl", SWAP)
    w_kv_all = over_seq(w_kv, kv_flip)
    w_q_all = over_seq(w_q, q_flip)

    def ring(own):
        half = own.shape[0] // 2
        left = lax.ppermute(own, "x", NEXT)
        right = lax.ppermute(own, "x", PREV)
        low, high = (left[:half], right[half:])
        low = lax.ppermute(low, "x", NEXT)
        high = lax.ppermute(high, "x", PREV)
        return left, right, low, high

    other = lax.ppermute(sorted_tokens, "zh", SWAP)
    left, right, low, high = ring(sorted_tokens)
    oleft, oright, olow, ohigh = ring(other)

    def square(piece):
        wide = piece.astype(f32)
        return jnp.sum(wide * wide, 1, keepdims=True)

    total = sum(square(p) for p in (sorted_tokens, left, right, other, oleft, oright))
    total_low, total_high = (square(low), square(high))
    total += jnp.concatenate([total_low, total_high], 0)
    total += jnp.concatenate([square(olow), square(ohigh)], 0)
    inverse = lax.rsqrt(total * (1.0 / MODEL) + NORM_EPS)
    y, zl, core = (lax.axis_index("y"), lax.axis_index("zl"), lax.axis_index("core"))
    groups = jnp.stack([z * 4 + (x + d) % 4 for z in (zh, 1 - zh) for d in (0, 3, 1, 2)])
    ids = jnp.stack([groups // 2, (groups % 2) ^ zl]).astype(jnp.int32)
    half = ROWS // 2
    pieces = [sorted_tokens, left, right, low, high, other, oleft, oright, olow, ohigh]
    slots = [(0, 0, ROWS), (1, 0, ROWS), (2, 0, ROWS), (3, 0, half), (3, half, half)]

    half_dim = HD // 2
    inv_freq = ROPE_BASE ** (-jnp.arange(half_dim, dtype=f32) * 2.0 / HD)
    angles = sorted_pos.astype(f32)[:, None] * inv_freq[None, :]
    cosine = jnp.cos(angles)
    sines = jnp.sin(angles)
    cosine = jnp.concatenate([cosine, cosine], 1)
    sines = jnp.concatenate([-sines, sines], 1)

    chips = [((y + d) % 4, f) for d in (0, 3, 1, 2) for f in (0, 1)]
    sources = jnp.stack([(a * 2 + c) * 2 + f for c in (core, 1 - core) for a, f in chips])
    pos_all = w_kv_all[:, :, :, ROWS : ROWS + 4].astype(jnp.int32).reshape(SOURCES, 2, ROWS)
    pos_all = pos_all[:, 0] * 128 + pos_all[:, 1]
    picked = sources[:, None] == jnp.arange(SOURCES)[None, :]
    pos_all = jnp.sum(jnp.where(picked[:, :, None], pos_all[None], 0), 1)
    kpos = pos_all.reshape(SOURCES, NSTEPS, KSTEP).transpose(1, 0, 2)
    first_pos = jnp.min(kpos, (1, 2))
    last_pos = jnp.max(kpos, (1, 2))
    kpos = kpos.reshape(NSTEPS, 1, KEYS)
    by_block = sorted_pos.reshape(BLOCKS, BLOCK)
    full = jnp.sum((last_pos[None, :] <= by_block[:, :1]).astype(jnp.int32), 1)
    need = jnp.sum((first_pos[None, :] <= by_block[:, -1:]).astype(jnp.int32), 1)
    bounds = jnp.stack([full, need])
    qpos = jnp.tile(by_block[:, None, :], (1, HEADS, 1)).reshape(BLOCKS, HEADS * BLOCK, 1)

    kv_bias = jnp.concatenate((b_key, b_value))[None, :]
    start = project(pieces[:5], slots, ids, w_kv_all, (), False, FIRST)
    inverse, kpos, bounds, qpos, start = lax.optimization_barrier(
        (inverse, kpos, bounds, qpos, start)
    )
    finish = (inverse, kv_bias, cosine, sines)
    kv = project(pieces[5:], slots, ids, w_kv_all, finish, False, LAST, start)

    pair = jnp.stack([kv, lax.ppermute(kv, "zl", SWAP)])
    own_kv = [pair] + [lax.ppermute(pair, "y", steps) for steps in (NEXT, PREV, ACROSS)]
    all_kv = own_kv + [lax.ppermute(a, "core", SWAP) for a in own_kv]

    finish = (inverse, b_query[None, :], cosine, sines)
    both_slots = slots + [(slot + 4, at, size) for slot, at, size in slots]
    queries = project(pieces, both_slots, ids, w_q_all, finish, True)

    mirrored = [
        ((yy * 4 + xx), (yy * 4 + (yy - xx) % 4)) for yy in range(4) for xx in range(4)
    ]
    moved = lax.ppermute(moved, ("y", "x"), mirrored)
    flip = lax.ppermute(moved, "zl", SWAP)
    moved, flip, _ = lax.optimization_barrier((moved, flip, all_kv[1:4]))
    w_out_all = over_seq(moved, flip)
    mix_ids = jnp.stack([(groups + x) % 4, (groups // 4) ^ zl]).astype(jnp.int32)

    base = tokens
    contexts, parts = ([], [])
    for first, count in CALLS:
        at = slice(first, first + count)
        parts.append(attend(bounds[:, at], queries, qpos, all_kv, kpos, first, count))
        if first + count == BLOCKS // 2 or first + count == BLOCKS:
            own = parts[0] if len(parts) == 1 else jnp.concatenate(parts, 0)
            contexts.append(own)
            parts = []
            last = first + count == BLOCKS
            half = BLOCKS // 2 if last else 0
            across = lax.ppermute(own, "zh", SWAP)
            near = [own] + [lax.ppermute(own, "x", s) for s in (NEXT, PREV, ACROSS)]
            far = [across] + [lax.ppermute(across, "x", s) for s in (NEXT, PREV)]
            found = near + far + [lax.ppermute(near[3], "zh", SWAP)]
            rows = slice(half * BLOCK, (first + count) * BLOCK)
            base = mix(found, mix_ids, w_out_all, back[:, rows], base, last)
    context = jnp.dot(back, jnp.concatenate(contexts, 0), preferred_element_type=f32).astype(bf16)
    return (base, context)


def solution(mesh):
    fine = Mesh(mesh.devices.reshape(4, 2, 2, 2, 4), SEQ + TENSOR)
    in_specs = (
        P(SEQ, TENSOR),
        P(SEQ),
        P(),
        P(SEQ, TENSOR),
        P(SEQ, TENSOR),
        P(SEQ, TENSOR),
        P(TENSOR),
        P(TENSOR),
        P(TENSOR),
        P(TENSOR, SEQ),
    )
    out_specs = (P(SEQ, TENSOR), P(SEQ, TENSOR))
    return jax.shard_map(block, mesh=fine, in_specs=in_specs, out_specs=out_specs, check_vma=False)
```

```python
import math

import jax
import jax.numpy as jnp
from jax import lax
from jax.experimental import pallas as pl
from jax.experimental.pallas import tpu as pltpu
from jax.sharding import Mesh, PartitionSpec as P


HD = 128
NORM_EPS = 1e-06
ROPE_BASE = 1000000.0
NEG_FILL = -1e30
SEQ = ("y", "zl", "core")
TENSOR = ("zh", "x")
ROWS = 512
FEAT = 1024
MODEL = 8192
SOURCES = 16
GROUPS = 8
HEADS = 4
POS_ROWS = 16
KSTEP = 64
NSTEPS = ROWS // KSTEP
KEYS = SOURCES * KSTEP
BLOCK = 128
BLOCKS = ROWS // BLOCK
CALLS = ((0, 2), (2, 2))
PER_DOT = 1
QSCALE = HD**-0.5 * math.log2(math.e)


IN_ORDER = ("arbitrary",)
FIRST, LAST = (1, 2)
NEXT = [(i, (i + 1) % 4) for i in range(4)]
PREV = [(i, (i - 1) % 4) for i in range(4)]
ACROSS = [(i, (i + 2) % 4) for i in range(4)]
SWAP = [(0, 1), (1, 0)]


def whole(*shape):
    return pl.BlockSpec(shape, lambda k, ids: (0,) * len(shape))


def add_squares(rows, square, started):
    wide = rows.astype(jnp.float32)
    wide = wide * wide
    total = wide[:, :HD]
    for i in range(1, rows.shape[1] // HD):
        total = total + wide[:, i * HD : (i + 1) * HD]
    square[...] = square[...] + total if started else total


def dots(
    ids, pieces, slots, w_ref, w_to, size, buffer, w_buffer, acc, sems, before=None, square=None
):
    groups = buffer.shape[1] // size
    made = []
    for i, (slot, start, count) in enumerate(slots):
        to = buffer.at[pl.ds(start, count), pl.ds(slot * size, size)]
        made.append((slot, pltpu.make_async_copy(pieces[i], to, sems.at[i])))
    for g in range(groups):
        for c in range(2):
            source = w_ref.at[ids[0, g], c, ids[1, g], pl.ds(0, ROWS)]
            sem = sems.at[len(slots) + g * 2 + c]
            made.append((g, pltpu.make_async_copy(source, w_to(w_buffer, g, c), sem)))
    made.sort(key=lambda pair: pair[0])
    for _, copy in made:
        copy.start()
    for k in range(groups // PER_DOT):
        for slot, copy in made:
            if slot // PER_DOT == k:
                copy.wait()
        deep = slice(k * PER_DOT * size, (k + 1) * PER_DOT * size)
        part = jnp.dot(buffer[:, deep], w_buffer[deep, :], preferred_element_type=jnp.float32)
        if k == 0:
            acc[...] = part if before is None else part + before[...]
        else:
            acc[...] += part
        if square is not None:
            add_squares(buffer[:, deep], square, k > 0)


def rows_to(w_buffer, g, c):
    return w_buffer.at[pl.ds((g * 2 + c) * ROWS, ROWS)]


def columns_to(w_buffer, g, c):
    return w_buffer.at[pl.ds(g * ROWS, ROWS), pl.ds(c * ROWS, ROWS)]


def project_body(slots, queries, partial, ids, *refs):
    pieces = refs[: len(slots)]
    w_ref = refs[len(slots)]
    refs = refs[len(slots) + 1 :]
    before, square = (None, None)
    if partial == FIRST:
        acc, square, buffer, w_buffer, sems = refs
    elif partial == LAST:
        before, early_ref, *refs = refs
        bias_ref, cos_ref, sin_ref, out_ref, square, buffer, w_buffer, acc, sems = refs
    else:
        square_ref, bias_ref, cos_ref, sin_ref, out_ref, buffer, w_buffer, acc, sems = refs
    dots(ids, pieces, slots, w_ref, rows_to, FEAT, buffer, w_buffer, acc, sems, before, square)
    if partial == FIRST:
        return
    if partial == LAST:
        square[...] += early_ref[...]
        square_ref = square
    mean = jnp.sum(square_ref[...], axis=1, keepdims=True) * (1.0 / MODEL)
    inverse = lax.rsqrt(mean + NORM_EPS)
    cosine = cos_ref[...]
    sines = sin_ref[...]

    def head(i):
        return acc[:, i * HD : (i + 1) * HD] * inverse + bias_ref[:, i * HD : (i + 1) * HD]

    def turned(u):
        return u * cosine + pltpu.roll(u, HD // 2, 1) * sines

    if queries:
        for i in range(HEADS):
            q = (turned(head(i)) * QSCALE).astype(jnp.bfloat16)
            for b in range(BLOCKS):
                out_ref[b, i * BLOCK : (i + 1) * BLOCK] = q[b * BLOCK : (b + 1) * BLOCK]
    else:
        out_ref[:, :HD] = turned(head(0)).astype(jnp.bfloat16)
        out_ref[:, HD:] = head(1).astype(jnp.bfloat16)


SCALARS = pl.BlockSpec(memory_space=pltpu.SMEM)
ANYWHERE = pl.BlockSpec(memory_space=pl.ANY)
NEAR = pl.BlockSpec(memory_space=pltpu.VMEM)


def project(pieces, slots, ids, weights, finish, queries, partial=None, before=None):
    width = HEADS * HD if queries else 2 * HD
    groups = GROUPS if partial is None else GROUPS // 2
    ids = ids[:, GROUPS - groups :] if partial == LAST else ids[:, :groups]
    dtype = jnp.bfloat16
    out_shape = (BLOCKS, HEADS * BLOCK, HD) if queries else (ROWS, 2 * HD)
    extra = finish if before is None else before + finish
    scratch = [
        pltpu.VMEM((ROWS, groups * FEAT), jnp.bfloat16),
        pltpu.VMEM((groups * FEAT, width), jnp.bfloat16),
    ]
    if partial == FIRST:
        out_shape, dtype = ((ROWS, width), jnp.float32)
    else:
        scratch += [pltpu.VMEM((ROWS, width), jnp.float32)]
    scratch += [pltpu.SemaphoreType.DMA((len(pieces) + 2 * groups,))]
    out = [jax.ShapeDtypeStruct(out_shape, dtype), jax.ShapeDtypeStruct((ROWS, HD), jnp.float32)]

    def body(*refs):
        project_body(slots, queries, partial, *refs)

    return pl.pallas_call(
        body,
        in_specs=[SCALARS] + [ANYWHERE] * (len(pieces) + 1) + [NEAR] * len(extra),
        out_specs=NEAR if queries else [NEAR, NEAR],
        scratch_shapes=scratch,
        out_shape=out[0] if queries else out,
        cost_estimate=pl.CostEstimate(
            flops=2 * ROWS * groups * FEAT * width, transcendentals=0, bytes_accessed=16 << 20
        ),
        name="pq" if queries else ("pk0" if partial == FIRST else "pk1"),
    )(ids, *pieces, weights, *extra)


def attend_body(first, bounds, q_ref, qpos_ref, kpos_ref, *refs):
    pairs = refs[: SOURCES // 2]
    out_ref, kv_ref, top, acc, sems = refs[SOURCES // 2 :]
    block_at = pl.program_id(0)
    full = bounds[0, block_at]
    need = bounds[1, block_at]

    def fetch(i):
        return pltpu.make_async_copy(pairs[i], kv_ref.at[pl.ds(2 * i, 2)], sems.at[i])

    @pl.when(block_at == 0)
    def _():
        for i in range(len(pairs)):
            fetch(i).start()

    top[...] = jnp.full_like(top, NEG_FILL)
    acc[...] = jnp.zeros_like(acc)

    @pl.when(block_at == 0)
    def _():
        for i in range(len(pairs)):
            fetch(i).wait()

    ones = jnp.ones((KEYS, HD), jnp.bfloat16)
    parts = top.shape[0]
    rows = top.shape[1]

    def one_step(j, masked):
        at = pl.multiple_of(j * KSTEP, KSTEP)
        block = kv_ref[:, pl.ds(at, KSTEP), :].reshape(KEYS, 2 * HD)
        keys = block[:, :HD]
        values = jnp.concatenate([block[:, HD:], ones], axis=1)

        def scores_of(h):
            return lax.dot_general(
                q_ref[0, h * rows : (h + 1) * rows],
                keys,
                (((1,), (1,)), ((), ())),
                preferred_element_type=jnp.float32,
            )

        following = scores_of(0)
        for h in range(parts):
            scores = following
            following = scores_of(h + 1) if h + 1 < parts else None
            if masked:
                row_pos = qpos_ref[0, h * rows : (h + 1) * rows]
                allowed = kpos_ref[j] <= jnp.concatenate([row_pos] * (KEYS // HD), axis=1)
                scores = jnp.where(allowed, scores, NEG_FILL)
            old = top[h]
            new = jnp.maximum(old, jnp.max(scores, axis=1, keepdims=True))
            weights = jnp.exp2(scores - jnp.concatenate([new] * (KEYS // HD), axis=1))
            rescale = jnp.exp2(old - new)
            top[h] = new
            acc[h] = acc[h] * jnp.concatenate([rescale, rescale], axis=1) + jnp.dot(
                weights.astype(jnp.bfloat16), values, preferred_element_type=jnp.float32
            )

    def unmasked(j, carry):
        one_step(j, False)
        return carry

    def masked(j, carry):
        one_step(j, True)
        return carry

    if first == 0:
        lax.fori_loop(0, need, masked, 0)
    else:
        lax.fori_loop(0, full, unmasked, 0)
        lax.fori_loop(full, need, masked, 0)
    for h in range(HEADS):
        part, at = (h * BLOCK // rows, h * BLOCK % rows)
        done = acc[part, at : at + BLOCK, :HD] / acc[part, at : at + BLOCK, HD:]
        out_ref[:, h * HD : (h + 1) * HD] = done.astype(jnp.bfloat16)


def attend(bounds, queries, qpos, pairs, kpos, first, count):
    part = 2 * BLOCK

    def body(*refs):
        attend_body(first, *refs)

    return pl.pallas_call(
        body,
        grid_spec=pltpu.PrefetchScalarGridSpec(
            num_scalar_prefetch=1,
            grid=(count,),
            in_specs=[
                pl.BlockSpec((1, HEADS * BLOCK, HD), lambda c, b: (c + first, 0, 0)),
                pl.BlockSpec((1, HEADS * BLOCK, HD), lambda c, b: (c + first, 0, 0)),
                whole(NSTEPS, 1, KEYS),
            ]
            + [pl.BlockSpec(memory_space=pl.ANY)] * len(pairs),
            out_specs=pl.BlockSpec((BLOCK, HEADS * HD), lambda c, b: (c, 0)),
            scratch_shapes=[
                pltpu.VMEM((SOURCES, ROWS, 2 * HD), jnp.bfloat16),
                pltpu.VMEM((HEADS * BLOCK // part, part, HD), jnp.float32),
                pltpu.VMEM((HEADS * BLOCK // part, part, 2 * HD), jnp.float32),
                pltpu.SemaphoreType.DMA((len(pairs),)),
            ],
        ),
        out_shape=jax.ShapeDtypeStruct((BLOCK * count, HEADS * HD), jnp.bfloat16),
        compiler_params=pltpu.CompilerParams(dimension_semantics=IN_ORDER),
        cost_estimate=pl.CostEstimate(
            flops=4 * HEADS * BLOCK * count * SOURCES * ROWS * HD,
            transcendentals=HEADS * BLOCK * count * SOURCES * ROWS,
            bytes_accessed=6 << 20,
        ),
    )(bounds, queries, qpos, kpos, *pairs)


def mix_body(slots, ids, *refs):
    pieces = refs[: len(slots)]
    refs = refs[len(slots) :]
    w_ref, back_ref, tokens_ref, out_ref, context_ref, buffer, w_buffer, acc, sems = refs
    dots(ids, pieces, slots, w_ref, columns_to, ROWS, buffer, w_buffer, acc, sems)
    back = back_ref[...]
    context = jnp.dot(back, buffer[:, :ROWS], preferred_element_type=jnp.float32)
    context_ref[...] = context.astype(jnp.bfloat16)
    high = acc[...].astype(jnp.bfloat16)
    low = (acc[...] - high.astype(jnp.float32)).astype(jnp.bfloat16)
    mixed = jnp.dot(back, high, preferred_element_type=jnp.float32) + jnp.dot(
        back, low, preferred_element_type=jnp.float32
    )
    out_ref[...] = (tokens_ref[...].astype(jnp.float32) + mixed).astype(jnp.bfloat16)


def mix(pieces, slots, ids, w_out, back, tokens):
    def body(*refs):
        mix_body(slots, *refs)

    return pl.pallas_call(
        body,
        in_specs=[SCALARS] + [ANYWHERE] * (len(pieces) + 1) + [NEAR] * 2,
        out_specs=[NEAR, NEAR],
        scratch_shapes=[
            pltpu.VMEM((ROWS, GROUPS * ROWS), jnp.bfloat16),
            pltpu.VMEM((GROUPS * ROWS, FEAT), jnp.bfloat16),
            pltpu.VMEM((ROWS, FEAT), jnp.float32),
            pltpu.SemaphoreType.DMA((len(pieces) + 2 * GROUPS,)),
        ],
        out_shape=[
            jax.ShapeDtypeStruct((ROWS, FEAT), jnp.bfloat16),
            jax.ShapeDtypeStruct((ROWS, HEADS * HD), jnp.bfloat16),
        ],
        cost_estimate=pl.CostEstimate(
            flops=2 * ROWS * HEADS * HD * GROUPS * FEAT, transcendentals=0, bytes_accessed=16 << 20
        ),
        name="m",
    )(ids, *pieces, w_out, back, tokens)


def block(tokens, positions, norm_gain, w_query, w_key, w_value, b_query, b_key, b_value, w_out):
    bf16, f32 = (jnp.bfloat16, jnp.float32)
    seq_at = lax.axis_index(SEQ)
    zh, x = (lax.axis_index("zh"), lax.axis_index("x"))

    spread = [
        (
            ((yy * 2 + zz) * 2 + hh) * 4 + xx,
            ((((yy % 2) * 2 + zz + xx) % 4 * 2 + hh) * 2 + yy // 2) * 4 + xx,
        )
        for yy in range(4)
        for zz in range(2)
        for hh in range(2)
        for xx in range(4)
    ]
    moved = lax.ppermute(w_out, ("y", "zl", "zh", "x"), spread)

    rank = jnp.sum((positions[None, :] < positions[:, None]).astype(jnp.int32), 1)
    chosen = rank[None, :] == jnp.arange(ROWS, dtype=jnp.int32)[:, None]
    order = chosen.astype(bf16)
    back = (rank[:, None] == jnp.arange(ROWS, dtype=jnp.int32)[None, :]).astype(bf16)
    sorted_pos = jnp.sum(jnp.where(chosen, positions[None, :], 0), 1)
    sorted_tokens = jnp.dot(order, tokens, preferred_element_type=f32).astype(bf16)

    gain = lax.dynamic_slice(norm_gain, (seq_at * ROWS,), (ROWS,))[:, None]
    w_kv = (jnp.concatenate((w_key, w_value), 1).astype(f32) * gain).astype(bf16)
    w_q = (w_query.astype(f32) * gain).astype(bf16)
    pos_rows = jnp.stack([sorted_pos >> 7, sorted_pos & 127]).astype(bf16)
    pos_rows = jnp.pad(pos_rows.reshape(4, 2 * HD), ((0, POS_ROWS - 4), (0, 0)))
    w_kv = jnp.concatenate([w_kv, pos_rows], 0)

    def over_seq(own, flip):
        both = jnp.concatenate([own, flip], 0)
        whole_seq = lax.all_gather(both, ("y", "core"), axis=0, tiled=True)
        return whole_seq.reshape((4, 2, 2) + own.shape)

    kv_flip = lax.ppermute(w_kv, "zl", SWAP)
    q_flip = lax.ppermute(w_q, "zl", SWAP)
    w_kv_all = over_seq(w_kv, kv_flip)
    w_q_all = over_seq(w_q, q_flip)

    def ring(own):
        half = own.shape[0] // 2
        left = lax.ppermute(own, "x", NEXT)
        right = lax.ppermute(own, "x", PREV)
        low, high = (left[:half], right[half:])
        low = lax.ppermute(low, "x", NEXT)
        high = lax.ppermute(high, "x", PREV)
        return left, right, low, high

    other = lax.ppermute(sorted_tokens, "zh", SWAP)
    left, right, low, high = ring(sorted_tokens)
    oleft, oright, olow, ohigh = ring(other)

    y, zl, core = (lax.axis_index("y"), lax.axis_index("zl"), lax.axis_index("core"))
    groups = jnp.stack([z * 4 + (x + d) % 4 for z in (zh, 1 - zh) for d in (0, 3, 1, 2)])
    ids = jnp.stack([groups // 2, (groups % 2) ^ zl]).astype(jnp.int32)
    half = ROWS // 2
    pieces = [sorted_tokens, left, right, low, high, other, oleft, oright, olow, ohigh]
    slots = [(0, 0, ROWS), (1, 0, ROWS), (2, 0, ROWS), (3, 0, half), (3, half, half)]

    half_dim = HD // 2
    inv_freq = ROPE_BASE ** (-jnp.arange(half_dim, dtype=f32) * 2.0 / HD)
    angles = sorted_pos.astype(f32)[:, None] * inv_freq[None, :]
    cosine = jnp.cos(angles)
    sines = jnp.sin(angles)
    cosine = jnp.concatenate([cosine, cosine], 1)
    sines = jnp.concatenate([-sines, sines], 1)

    chips = [((y + d) % 4, f) for d in (0, 3, 1, 2) for f in (0, 1)]
    sources = jnp.stack([(a * 2 + c) * 2 + f for c in (core, 1 - core) for a, f in chips])
    pos_all = w_kv_all[:, :, :, ROWS : ROWS + 4].astype(jnp.int32).reshape(SOURCES, 2, ROWS)
    pos_all = pos_all[:, 0] * 128 + pos_all[:, 1]
    picked = sources[:, None] == jnp.arange(SOURCES)[None, :]
    pos_all = jnp.sum(jnp.where(picked[:, :, None], pos_all[None], 0), 1)
    kpos = pos_all.reshape(SOURCES, NSTEPS, KSTEP).transpose(1, 0, 2)
    first_pos = jnp.min(kpos, (1, 2))
    last_pos = jnp.max(kpos, (1, 2))
    kpos = kpos.reshape(NSTEPS, 1, KEYS)
    by_block = sorted_pos.reshape(BLOCKS, BLOCK)
    full = jnp.sum((last_pos[None, :] <= by_block[:, :1]).astype(jnp.int32), 1)
    need = jnp.sum((first_pos[None, :] <= by_block[:, -1:]).astype(jnp.int32), 1)
    bounds = jnp.stack([full, need])
    qpos = jnp.broadcast_to(by_block[:, None, :, None], (BLOCKS, HEADS, BLOCK, HD))
    qpos = qpos.reshape(BLOCKS, HEADS * BLOCK, HD)

    kv_bias = jnp.concatenate((b_key, b_value))[None, :]
    kpos, bounds, qpos, ids = lax.optimization_barrier((kpos, bounds, qpos, ids))
    early = tuple(project(pieces[:5], slots, ids, w_kv_all, (), False, FIRST))
    finish = (kv_bias, cosine, sines)
    kv, square = project(pieces[5:], slots, ids, w_kv_all, finish, False, LAST, early)

    pair = jnp.stack([kv, lax.ppermute(kv, "zl", SWAP)])
    own_kv = [pair] + [lax.ppermute(pair, "y", steps) for steps in (NEXT, PREV, ACROSS)]
    all_kv = own_kv + [lax.ppermute(a, "core", SWAP) for a in own_kv]

    finish = (square, b_query[None, :], cosine, sines)
    both_slots = slots + [(slot + 4, at, size) for slot, at, size in slots]
    queries = project(pieces, both_slots, ids, w_q_all, finish, True)

    mirrored = [
        ((yy * 4 + xx), (yy * 4 + (yy - xx) % 4)) for yy in range(4) for xx in range(4)
    ]
    moved = lax.ppermute(moved, ("y", "x"), mirrored)
    flip = lax.ppermute(moved, "zl", SWAP)
    moved, flip, _ = lax.optimization_barrier((moved, flip, all_kv[1:4]))
    w_out_all = over_seq(moved, flip)
    mix_ids = jnp.stack([(groups + x) % 4, (groups // 4) ^ zl]).astype(jnp.int32)

    found, mix_slots = ([], [])
    for first, count in CALLS:
        at = slice(first, first + count)
        own = attend(bounds[:, at], queries, qpos, all_kv, kpos, first, count)
        across = lax.ppermute(own, "zh", SWAP)
        near = [own] + [lax.ppermute(own, "x", s) for s in (NEXT, PREV, ACROSS)]
        far = [across] + [lax.ppermute(across, "x", s) for s in (NEXT, PREV)]
        found += near + far + [lax.ppermute(near[3], "zh", SWAP)]
        mix_slots += [(i, first * BLOCK, count * BLOCK) for i in range(GROUPS)]
    return tuple(mix(found, mix_slots, mix_ids, w_out_all, back, tokens))


def solution(mesh):
    fine = Mesh(mesh.devices.reshape(4, 2, 2, 2, 4), SEQ + TENSOR)
    in_specs = (
        P(SEQ, TENSOR),
        P(SEQ),
        P(),
        P(SEQ, TENSOR),
        P(SEQ, TENSOR),
        P(SEQ, TENSOR),
        P(TENSOR),
        P(TENSOR),
        P(TENSOR),
        P(TENSOR, SEQ),
    )
    out_specs = (P(SEQ, TENSOR), P(SEQ, TENSOR))
    return jax.shard_map(block, mesh=fine, in_specs=in_specs, out_specs=out_specs, check_vma=False)
```
